256 devices in a mesh: gx: 4 (over x), gy: 8 (over y, core), ha: 8 (over z).
Axes of the slice: x: 4, y: 4, z: 8, core: 2. Of those that a mesh axis runs over, the one named last changes fastest.
Arguments:
- level_set: float32 [32, 128, 80, 128], P('gx', 'gy', 'ha'), may hold values from -4 to 4
- wind_field: float32 [2, 32, 128], P(None, 'gx', 'gy'), may hold values from -3 to 3
Outputs:
- increment: float32 [32, 128, 80, 128], P('gx', 'gy', 'ha')
The draws below stay inside these ranges and needn't reach their ends.
All inputs are finite; a program needn't handle non-finite values.
Results may differ from the reference program's by a relative error of at most 0.000073.
Values sent between devices are 32-bit elements; how exact they have to be, the bound alone decides.
A program may use at most 128 MiB of HBM per device.

```python
import math
import jax
import jax.numpy as jnp
from jax import lax

NV = 128
NX = 32
NY = 128
NH = 80


CELL_SIZE = 0.05


def draw_level_set(key, part):
    rough_key = jax.random.fold_in(key, 11)
    center_key = jax.random.fold_in(key, 12)
    shape = (NX, NY, NH, NV)
    centers = jax.random.uniform(center_key, (2,), jnp.float32, 0.3, 0.7)
    pos_x = (jnp.arange(NX, dtype=jnp.float32) + 0.5) / NX
    pos_y = (jnp.arange(NY, dtype=jnp.float32) + 0.5) / NY
    span_x = (pos_x - centers[0]) * NX * CELL_SIZE
    span_y = (pos_y - centers[1]) * NY * CELL_SIZE
    smooth = jnp.sqrt(span_x[:, None] ** 2 + span_y[None, :] ** 2 + 0.01) - 0.25 * NX * CELL_SIZE
    smooth = smooth[:, :, None, None]
    rough = 0.5 * jax.random.normal(rough_key, shape, jnp.float32)
    surface = rough + smooth
    return jnp.clip(surface, -4.0, 4.0)


def draw_wind_field(key, part):
    raw_key = jax.random.fold_in(key, 21)
    shape = (2, NX, NY)
    ramp = 0.1 + 2.9 * (jnp.arange(NX, dtype=jnp.float32) + 0.5) / NX
    raw = jax.random.uniform(raw_key, shape, jnp.float32, -1.0, 1.0)
    return raw * ramp[None, :, None]


def setup_inputs(seed: int = 0) -> dict:
    streams_of = jax.random.split(jax.random.key(seed), 3)
    return {
        "level_set": draw_level_set(jax.random.fold_in(streams_of[2], 71), 0),
        "wind_field": draw_wind_field(jax.random.fold_in(streams_of[2], 71), 0),
    }


CELL_SIZE = 0.05
SPEED_LOW = 0.1
SPEED_SPAN = 0.4
TURN_MAX = 1.0
ACCEL_MAX = 0.05
CFL_NUMBER = 0.5
WENO_EPS = 1e-6


def ghost_rows(values, along, at_low):
    length = values.shape[along]
    if at_low:
        edge_row = lax.slice_in_dim(values, 0, 1, axis=along)
        next_row = lax.slice_in_dim(values, 1, 2, axis=along)
        reaches = (3.0, 2.0, 1.0)
    else:
        edge_row = lax.slice_in_dim(values, length - 1, length, axis=along)
        next_row = lax.slice_in_dim(values, length - 2, length - 1, axis=along)
        reaches = (1.0, 2.0, 3.0)
    slope_edge = edge_row - next_row
    return jnp.concatenate([edge_row + distance * slope_edge for distance in reaches], axis=along)


def extend(values, along):
    return jnp.concatenate([ghost_rows(values, along, True), values, ghost_rows(values, along, False)], axis=along)


def speed_shifts(values):
    length = values.shape[3]
    below_rows = ghost_rows(values, 3, True)
    above_rows = ghost_rows(values, 3, False)
    shifted = []
    for displace in range(-3, 4):
        pieces = []
        if displace < 0:
            pieces.append(lax.slice_in_dim(below_rows, 3 + displace, 3, axis=3))
        pieces.append(lax.slice_in_dim(values, max(displace, 0), length + min(displace, 0), axis=3))
        if displace > 0:
            pieces.append(lax.slice_in_dim(above_rows, 0, displace, axis=3))
        shifted.append(jnp.concatenate(pieces, axis=3) if len(pieces) > 1 else pieces[0])
    return shifted


def weno_side(left_far, left_near, middle, right_near, right_far):
    guess_one = left_far * (1.0 / 3.0) - left_near * (7.0 / 6.0) + middle * (11.0 / 6.0)
    guess_two = -left_near * (1.0 / 6.0) + middle * (5.0 / 6.0) + right_near * (1.0 / 3.0)
    guess_three = middle * (1.0 / 3.0) + right_near * (5.0 / 6.0) - right_far * (1.0 / 6.0)
    smooth_one = (13.0 / 12.0) * jnp.square(left_far - 2.0 * left_near + middle) + 0.25 * jnp.square(left_far - 4.0 * left_near + 3.0 * middle)
    smooth_two = (13.0 / 12.0) * jnp.square(left_near - 2.0 * middle + right_near) + 0.25 * jnp.square(left_near - right_near)
    smooth_three = (13.0 / 12.0) * jnp.square(middle - 2.0 * right_near + right_far) + 0.25 * jnp.square(3.0 * middle - 4.0 * right_near + right_far)
    weight_one = 0.1 / jnp.square(smooth_one + WENO_EPS)
    weight_two = 0.6 / jnp.square(smooth_two + WENO_EPS)
    weight_three = 0.3 / jnp.square(smooth_three + WENO_EPS)
    return (weight_one * guess_one + weight_two * guess_two + weight_three * guess_three) / (weight_one + weight_two + weight_three)


def weno_pair(shifted, spacing):
    slopes = [(shifted[position + 1] - shifted[position]) / spacing for position in range(6)]
    left_slope = weno_side(slopes[0], slopes[1], slopes[2], slopes[3], slopes[4])
    right_slope = weno_side(slopes[5], slopes[4], slopes[3], slopes[2], slopes[1])
    return left_slope, right_slope


def cell_rates(cos_head, sin_head, speeds, wind_x, wind_y, d_theta, d_speed):
    along_x = speeds[None, None, None, :] * cos_head[None, None, :, None] + wind_x[:, :, None, None]
    along_y = speeds[None, None, None, :] * sin_head[None, None, :, None] + wind_y[:, :, None, None]
    return jnp.abs(along_x) / CELL_SIZE + jnp.abs(along_y) / CELL_SIZE + TURN_MAX / d_theta + ACCEL_MAX / d_speed


def hamilton(x_pair, y_pair, head_pair, speed_pair, cos_head, sin_head, speeds, wind_x, wind_y):
    flow_x = speeds[None, None, None, :] * cos_head[None, None, :, None] + wind_x[:, :, None, None]
    flow_y = speeds[None, None, None, :] * sin_head[None, None, :, None] + wind_y[:, :, None, None]
    mean_x = 0.5 * (x_pair[0] + x_pair[1])
    mean_y = 0.5 * (y_pair[0] + y_pair[1])
    mean_head = 0.5 * (head_pair[0] + head_pair[1])
    mean_speed = 0.5 * (speed_pair[0] + speed_pair[1])
    value = -(flow_x * mean_x + flow_y * mean_y + TURN_MAX * jnp.abs(mean_head) + ACCEL_MAX * jnp.abs(mean_speed))
    damping = 0.5 * (jnp.abs(flow_x) * (x_pair[1] - x_pair[0]) + jnp.abs(flow_y) * (y_pair[1] - y_pair[0])
                     + TURN_MAX * (head_pair[1] - head_pair[0]) + ACCEL_MAX * (speed_pair[1] - speed_pair[0]))
    return -jnp.maximum(value - damping, 0.0)


def reference(level_set, wind_field):
    d_theta = 2.0 * math.pi / NH
    d_speed = SPEED_SPAN / NV
    angles = jnp.arange(NH, dtype=jnp.int32).astype(jnp.float32) * d_theta
    cos_head = jnp.cos(angles)
    sin_head = jnp.sin(angles)
    speeds = SPEED_LOW + SPEED_SPAN * (jnp.arange(NV, dtype=jnp.int32).astype(jnp.float32) + 0.5) / NV
    rows_all = jnp.arange(NX, dtype=jnp.int32)

    def plane_max(position):
        winds = lax.dynamic_slice_in_dim(wind_field, position, 1, 1)
        return jnp.max(cell_rates(cos_head, sin_head, speeds, winds[0], winds[1], d_theta, d_speed))

    time_step = CFL_NUMBER / jnp.max(lax.map(plane_max, rows_all))

    def advance(surface):
        x_padded = extend(surface, 0)

        def one_plane(position):
            x_plane = lax.dynamic_slice_in_dim(surface, position, 1, 0)
            x_shifted = [lax.dynamic_slice_in_dim(x_padded, position + 3 + displace, 1, 0) for displace in range(-3, 4)]
            y_padded = extend(x_plane, 1)
            y_shifted = [y_padded[:, 3 + displace:3 + displace + NY] for displace in range(-3, 4)]
            head_padded = jnp.concatenate([x_plane[:, :, NH - 3:], x_plane, x_plane[:, :, :3]], axis=2)
            head_shifted = [head_padded[:, :, 3 + displace:3 + displace + NH] for displace in range(-3, 4)]
            winds = lax.dynamic_slice_in_dim(wind_field, position, 1, 1)
            return hamilton(weno_pair(x_shifted, CELL_SIZE), weno_pair(y_shifted, CELL_SIZE),
                            weno_pair(head_shifted, d_theta), weno_pair(speed_shifts(x_plane), d_speed),
                            cos_head, sin_head, speeds, winds[0], winds[1])

        return lax.map(one_plane, rows_all).reshape(surface.shape)

    section_one = level_set + time_step * advance(level_set)
    section_two = 0.75 * level_set + 0.25 * (section_one + time_step * advance(section_one))
    advanced = (1.0 / 3.0) * level_set + (2.0 / 3.0) * (section_two + time_step * advance(section_two))
    return advanced - level_set
```

```python
import functools
import math

import jax
import jax.numpy as jnp
import numpy as np
from jax import lax
from jax.experimental import pallas as pl
from jax.experimental.pallas import tpu as pltpu
from jax.sharding import PartitionSpec as P

CELL_SIZE = 0.05
SPEED_LOW = 0.1
SPEED_SPAN = 0.4
TURN_MAX = 1.0
ACCEL_MAX = 0.05
CFL_NUMBER = 0.5
WENO_EPS = 1e-06
SCALE = 64.0
MESH = pl.DeviceIdType.MESH


def eps_of(spacing):
    return 0.75 * WENO_EPS * (spacing * SCALE) ** 2


def one_side(b1, b2, b3, t1, t2):
    c1 = 3.0 * b1
    c3 = b3 + b3
    return b2 * (c3 * t1 + c1 * t2) / (b2 * (b3 + c1) + c1 * c3)


def both_sides(p, c, m, ta, tb):
    x = m * ta
    y = p * tb
    twice = 2.0 * (x + y)
    p2 = p + p
    m2 = m + m
    total = p + m
    far = 3.0 * (p2 * m)
    left = c * (twice + y) / (c * (total + p2) + far)
    right = c * (twice + x) / (c * (total + m2) + far)
    return left, right


def along(u, eps):
    n = len(u)
    q = [u[k + 1] - u[k] for k in range(n - 1)]
    d = [q[k + 1] - q[k] for k in range(n - 2)]
    s = [None] + [d[k] - d[k - 1] for k in range(1, n - 2)]
    t = [None] + [s[k + 1] - s[k] for k in range(1, n - 3)]
    z = [1.5 * (e * e) for e in d]
    p, c, m = [None], [None], [None]
    for k in range(1, n - 2):
        v = s[k] * s[k] + eps
        x = 0.75 * (d[k - 1] * d[k])
        w = v - x
        c.append(v + x)
        p.append(w + z[k])
        m.append(w + z[k - 1])
    return d, s, t, p, c, m


def kernel(
    sizes,
    u_hbm,
    wind,
    out_hbm,
    u0,
    u1,
    u2,
    acc,
    fx2,
    fx6,
    fy2,
    fy6,
    xlo,
    xhi,
    hlo,
    hhi,
    ylo,
    yhi,
    ysend,
    cos_t,
    sin_t,
    wx,
    wy,
    step_buf,
    top_x,
    top_y,
    top_send,
    out_v,
    in_sem,
    out_sem,
    x_send,
    x_recv,
    h_send,
    h_recv,
    y_send,
    y_recv,
    top_send_sem,
    top_recv_sem,
):
    gx_n, gy_n, ha_n, nx, nh, ny, nv = sizes
    n_head = nh * ha_n
    d_theta = 2.0 * math.pi / n_head
    d_speed = SPEED_SPAN / nv
    gx, gy, ha = lax.axis_index("gx"), lax.axis_index("gy"), lax.axis_index("ha")
    below_x, above_x = gx > 0, gx < gx_n - 1
    below_y, above_y = gy > 0, gy < gy_n - 1
    h_up, h_down = lax.rem(ha + 1, ha_n), lax.rem(ha + ha_n - 1, ha_n)
    us = (u0, u1, u2)
    halves = ny // 8

    load_in = pltpu.make_async_copy(u_hbm, acc, in_sem.at[0])
    load_in.start()

    barrier = pltpu.get_barrier_semaphore()
    for k in range(1, gx_n):
        pl.semaphore_signal(barrier, inc=1, device_id={"gx": lax.rem(gx + k, gx_n)}, device_id_type=MESH)
    for k in range(1, gy_n):
        pl.semaphore_signal(barrier, inc=1, device_id={"gy": lax.rem(gy + k, gy_n)}, device_id_type=MESH)
    pl.semaphore_signal(barrier, inc=1, device_id={"ha": h_up}, device_id_type=MESH)
    pl.semaphore_signal(barrier, inc=1, device_id={"ha": h_down}, device_id_type=MESH)

    def rows(h):
        return pl.ds(8 + 8 * h, 8)

    def inner(h):
        return pl.ds(8 * h, 8)

    def x_copies(s, h):
        u = us[s]
        down = pltpu.make_async_remote_copy(
            src_ref=u.at[pl.ds(0, 3), :, rows(h), :], dst_ref=xhi.at[s, h],
            send_sem=x_send.at[s, h, 0], recv_sem=x_recv.at[s, h, 0],
            device_id={"gx": gx - 1}, device_id_type=MESH)
        up = pltpu.make_async_remote_copy(
            src_ref=u.at[pl.ds(nx - 3, 3), :, rows(h), :], dst_ref=xlo.at[s, h],
            send_sem=x_send.at[s, h, 1], recv_sem=x_recv.at[s, h, 1],
            device_id={"gx": gx + 1}, device_id_type=MESH)
        return down, up

    def h_copies(s, h):
        u = us[s]
        down = pltpu.make_async_remote_copy(
            src_ref=u.at[:, pl.ds(0, 3), rows(h), :], dst_ref=hhi.at[s, h],
            send_sem=h_send.at[s, h, 0], recv_sem=h_recv.at[s, h, 0],
            device_id={"ha": h_down}, device_id_type=MESH)
        up = pltpu.make_async_remote_copy(
            src_ref=u.at[:, pl.ds(nh - 3, 3), rows(h), :], dst_ref=hlo.at[s, h],
            send_sem=h_send.at[s, h, 1], recv_sem=h_recv.at[s, h, 1],
            device_id={"ha": h_up}, device_id_type=MESH)
        return down, up

    def y_copies(s):
        down = pltpu.make_async_remote_copy(
            src_ref=ysend.at[s, 0], dst_ref=yhi.at[s],
            send_sem=y_send.at[s, 0], recv_sem=y_recv.at[s, 0],
            device_id={"gy": gy - 1}, device_id_type=MESH)
        up = pltpu.make_async_remote_copy(
            src_ref=ysend.at[s, 1], dst_ref=ylo.at[s],
            send_sem=y_send.at[s, 1], recv_sem=y_recv.at[s, 1],
            device_id={"gy": gy + 1}, device_id_type=MESH)
        return down, up

    def start_half(s, h):
        down, up = x_copies(s, h)
        pl.when(below_x)(down.start)
        pl.when(above_x)(up.start)
        down, up = h_copies(s, h)
        down.start()
        up.start()
        copies = y_copies(s)
        if h == 0:
            pl.when(below_y)(copies[0].start)
        if h == halves - 1:
            pl.when(above_y)(copies[1].start)

    angles = lax.broadcasted_iota(jnp.int32, (n_head, nv), 0).astype(jnp.float32) * d_theta
    cos_t[...] = jnp.cos(angles)
    sin_t[...] = jnp.sin(angles)
    diagonal = lax.broadcasted_iota(jnp.int32, (ny, ny), 0) == lax.broadcasted_iota(jnp.int32, (ny, ny), 1)
    for i in range(nx):
        for part, out in ((0, wx), (1, wy)):
            row = jnp.broadcast_to(wind[part, pl.ds(i, 1), :], (ny, ny))
            column = jnp.sum(jnp.where(diagonal, row, 0.0), axis=1, keepdims=True)
            out[i] = jnp.broadcast_to(column, (ny, nv))

    low = np.float32(SPEED_LOW) + np.float32(SPEED_SPAN) * np.float32(0.5) / np.float32(nv)
    high = np.float32(SPEED_LOW) + np.float32(SPEED_SPAN) * np.float32(nv - 0.5) / np.float32(nv)
    wind_x, wind_y = wind[0], wind[1]

    def rate_of(k, top):
        c = jnp.broadcast_to(cos_t[pl.ds(k, 1), 0:ny], (nx, ny))
        n = jnp.broadcast_to(sin_t[pl.ds(k, 1), 0:ny], (nx, ny))
        for speed in (float(low), float(high)):
            top = jnp.maximum(top, jnp.abs(speed * c + wind_x) + jnp.abs(speed * n + wind_y))
        return top

    top = lax.fori_loop(0, n_head, rate_of, jnp.zeros((nx, ny), jnp.float32), unroll=4)
    top_send[0] = jnp.full((8, nv), jnp.max(top), jnp.float32)

    speeds = SPEED_LOW + SPEED_SPAN * (
        lax.broadcasted_iota(jnp.int32, (1, nv), 1).astype(jnp.float32) + 0.5) / nv

    def flow_of(j, carry):
        c = speeds * cos_t[pl.ds(ha * nh + j, 1), :]
        n = speeds * sin_t[pl.ds(ha * nh + j, 1), :]
        for i in range(nx):
            f = c + wx[i]
            fx2[i, j] = f * (0.5 / CELL_SIZE)
            fx6[i, j] = jnp.abs(f) * (1.0 / (6.0 * CELL_SIZE))
            f = n + wy[i]
            fy2[i, j] = f * (0.5 / CELL_SIZE)
            fy6[i, j] = jnp.abs(f) * (1.0 / (6.0 * CELL_SIZE))
        return carry

    lax.fori_loop(0, nh, flow_of, 0)

    load_in.wait()

    def pack_y(s, i):
        u = us[s]
        for j in range(nh):
            ysend[s, 0, i, pl.ds(3 * j, 3), :] = u[i, j, pl.ds(8, 3), :]
            ysend[s, 1, i, pl.ds(3 * j, 3), :] = u[i, j, pl.ds(8 + ny - 3, 3), :]

    def scale_in(i, carry):
        for j in range(nh):
            u0[i, j, pl.ds(8, ny), :] = acc[i, j] * SCALE
        return carry

    lax.fori_loop(0, nx, scale_in, 0)

    def pack_all(s):
        def body(i, carry):
            pack_y(s, i)
            return carry
        lax.fori_loop(0, nx, body, 0)

    pack_all(0)

    pl.semaphore_wait(barrier, gx_n - 1 + gy_n - 1 + 2)
    for h in range(halves):
        start_half(0, h)

    def top_copy(axis, me, size, k, phase):
        buf = (top_x, top_y)[phase]
        return pltpu.make_async_remote_copy(
            src_ref=top_send.at[phase], dst_ref=buf.at[k - 1],
            send_sem=top_send_sem.at[phase, k - 1], recv_sem=top_recv_sem.at[phase, k - 1],
            device_id={axis: lax.rem(me + k, size)}, device_id_type=MESH)

    top_copies = [
        [top_copy("gx", gx, gx_n, k, 0) for k in range(1, gx_n)],
        [top_copy("gy", gy, gy_n, k, 1) for k in range(1, gy_n)],
    ]
    for copy in top_copies[0]:
        copy.start()

    lane = lax.broadcasted_iota(jnp.int32, (8, nv), 1)
    first, last = lane == 0, lane == nv - 1

    def v_term(u):
        eps = eps_of(d_speed)
        e2 = eps * eps
        a = pltpu.roll(u, nv - 1, 1) - u
        b = u - pltpu.roll(u, 1, 1)
        q1 = jnp.where(last, b, a)
        q0 = jnp.where(first, a, b)
        d3 = 3.0 * (q0 + q1)
        d = q1 - q0
        dm = pltpu.roll(d, 1, 1)
        s = d - dm
        ta = s - pltpu.roll(s, 1, 1)
        tb = pltpu.roll(ta, nv - 1, 1)
        v = s * s + eps
        x = 0.75 * (d * dm)
        w = v - x
        c = v + x
        p = w + 1.5 * (d * d)
        m = w + 1.5 * (dm * dm)
        p = pltpu.roll(p * p, 1, 1)
        m = pltpu.roll(m * m, nv - 1, 1)
        c = c * c
        left = one_side(jnp.where(first, e2, p), c, m, jnp.where(first, 0.0, ta), tb)
        right = one_side(jnp.where(first, e2, m), c, p, jnp.where(first, 0.0, tb), ta)
        right = pltpu.roll(right - s, nv - 1, 1)
        return (ACCEL_MAX / (6.0 * d_speed)) * jnp.maximum(d3 + right, left + s - d3)

    def v_pass(s):
        u = us[s]

        def body(i, carry):
            for j in range(nh):
                for h in range(halves):
                    acc[i, j, inner(h), :] = v_term(u[i, j, rows(h), :])
            return carry

        lax.fori_loop(0, nx, body, 0)

    def h_pass(s, h):
        u = us[s]
        factor = TURN_MAX / (6.0 * d_theta)

        def body(i, carry):
            cells = [hlo[s, h, i, k] for k in range(3)]
            cells += [u[i, k, rows(h), :] for k in range(nh)]
            cells += [hhi[s, h, i, k] for k in range(3)]
            d, sd, t, p, c, m = along(cells, eps_of(d_theta))
            square = lambda r: [None] + [e * e for e in r[1:]]
            p, c, m = square(p), square(c), square(m)
            sides = {}
            for k in range(2, nh + 3):
                sides[k] = both_sides(p[k - 1], c[k], m[k + 1], t[k - 1], t[k])
            for j in range(nh):
                k = j + 2
                d3 = 3.0 * (cells[j + 4] - cells[j + 2])
                value = jnp.maximum(d3 + (sides[k + 1][1] - sd[k + 1]), (sides[k][0] + sd[k]) - d3)
                acc[i, j, inner(h), :] += factor * value
            return carry

        lax.fori_loop(0, nx, body, 0)

    def x_pass(s, h):
        u = us[s]

        def body(j, carry):
            cells = [xlo[s, h, k, j] for k in range(3)]
            cells += [u[k, j, rows(h), :] for k in range(nx)]
            cells += [xhi[s, h, k, j] for k in range(3)]
            d, sd, t, p, c, m = along(cells, eps_of(CELL_SIZE))
            for i in range(nx):
                k = i + 2
                f2 = fx2[i, j, inner(h), :]
                ahead = f2 > 0.0
                b1 = jnp.where(ahead, m[k + 2], p[k - 1])
                b2 = jnp.where(ahead, c[k + 1], c[k])
                b3 = jnp.where(ahead, p[k], m[k + 1])
                t1 = jnp.where(ahead, t[k + 1], t[k - 1])
                dd = d[k] - jnp.where(ahead, d[k + 1], d[k - 1])
                fix = one_side(b1 * b1, b2 * b2, b3 * b3, t1, t[k])
                acc[i, j, inner(h), :] += f2 * (cells[i + 4] - cells[i + 2]) + fx6[i, j, inner(h), :] * (dd + fix)
            return carry

        lax.fori_loop(0, nh, body, 0)

    def y_term(u, i, j, h):
        eps = eps_of(CELL_SIZE)
        f2 = fy2[i, j, inner(h), :]
        ahead = f2 > 0.0
        cells = [u[i, j, pl.ds(8 + 8 * h + r, 8), :] for r in range(-3, 4)]
        q = [cells[k + 1] - cells[k] for k in range(6)]
        d = [q[k + 1] - q[k] for k in range(5)]
        e1 = jnp.where(ahead, d[4], d[0])
        e2 = jnp.where(ahead, d[3], d[1])
        e3 = d[2]
        e4 = jnp.where(ahead, d[1], d[3])
        s1, s2, s3 = e2 - e1, e3 - e2, e4 - e3
        e2k, e3k = 0.75 * e2, 0.75 * e3
        b1 = (s1 * s1 + eps) + e2k * (e2 + s1)
        b2 = (s2 * s2 + eps) + e2k * e3
        b3 = (s3 * s3 + eps) + e3k * (e3 - s3)
        fix = one_side(b1 * b1, b2 * b2, b3 * b3, s2 - s1, s3 - s2)
        return f2 * (cells[4] - cells[2]) + fy6[i, j, inner(h), :] * (s2 + fix)

    def y_pass(s, h):
        u = us[s]
        dt = step_buf[...]

        def body(i, carry):
            for j in range(nh):
                total = acc[i, j, inner(h), :] + y_term(u, i, j, h)
                change = dt * jnp.minimum(total, 0.0)
                if s == 0:
                    u1[i, j, rows(h), :] = u0[i, j, rows(h), :] + change
                elif s == 1:
                    u2[i, j, rows(h), :] = 0.75 * u0[i, j, rows(h), :] + 0.25 * (u1[i, j, rows(h), :] + change)
                else:
                    out_v[i, j, inner(h), :] = (2.0 / 3.0 / SCALE) * ((u2[i, j, rows(h), :] - u0[i, j, rows(h), :]) + change)
            return carry

        lax.fori_loop(0, nx, body, 0)

    def receive_x(s, h):
        u = us[s]
        down, up = x_copies(s, h)
        pl.when(above_x)(down.wait_recv)
        pl.when(below_x)(up.wait_recv)

        @pl.when(jnp.logical_not(below_x))
        def _():
            def body(j, carry):
                edge = u[0, j, rows(h), :]
                slope = edge - u[1, j, rows(h), :]
                for r in (1, 2, 3):
                    xlo[s, h, 3 - r, j] = edge + float(r) * slope
                return carry
            lax.fori_loop(0, nh, body, 0)

        @pl.when(jnp.logical_not(above_x))
        def _():
            def body(j, carry):
                edge = u[nx - 1, j, rows(h), :]
                slope = edge - u[nx - 2, j, rows(h), :]
                for r in (1, 2, 3):
                    xhi[s, h, r - 1, j] = edge + float(r) * slope
                return carry
            lax.fori_loop(0, nh, body, 0)

    def receive_h(s, h):
        for copy in h_copies(s, h):
            copy.wait_recv()

    def receive_y(s, which):
        u = us[s]
        copy = y_copies(s)[which]
        there = (above_y, below_y)[which]

        @pl.when(there)
        def _():
            copy.wait_recv()

            def body(i, carry):
                for j in range(nh):
                    if which == 0:
                        u[i, j, pl.ds(8 + ny, 3), :] = yhi[s, i, pl.ds(3 * j, 3), :]
                    else:
                        u[i, j, pl.ds(5, 3), :] = ylo[s, i, pl.ds(3 * j, 3), :]
                return carry
            lax.fori_loop(0, nx, body, 0)

        @pl.when(jnp.logical_not(there))
        def _():
            def body(i, carry):
                for j in range(nh):
                    if which == 0:
                        edge = u[i, j, pl.ds(8 + ny - 1, 1), :]
                        slope = edge - u[i, j, pl.ds(8 + ny - 2, 1), :]
                        for r in (1, 2, 3):
                            u[i, j, pl.ds(8 + ny - 1 + r, 1), :] = edge + float(r) * slope
                    else:
                        edge = u[i, j, pl.ds(8, 1), :]
                        slope = edge - u[i, j, pl.ds(9, 1), :]
                        for r in (1, 2, 3):
                            u[i, j, pl.ds(8 - r, 1), :] = edge + float(r) * slope
                return carry
            lax.fori_loop(0, nx, body, 0)

    out_copies = []
    for s in range(3):
        v_pass(s)
        if s == 0:
            for copy in top_copies[0]:
                copy.wait_recv()
            best = top_send[0]
            for k in range(1, gx_n):
                best = jnp.maximum(best, top_x[k - 1])
            top_send[1] = best
            for copy in top_copies[1]:
                copy.start()
        for h in range(halves):
            receive_h(s, h)
            h_pass(s, h)
            receive_x(s, h)
            x_pass(s, h)
            if h == 0:
                receive_y(s, 1)
            if h == halves - 1:
                receive_y(s, 0)
            if s == 0 and h == 0:
                for copy in top_copies[1]:
                    copy.wait_recv()
                best = top_send[1]
                for k in range(1, gy_n):
                    best = jnp.maximum(best, top_y[k - 1])
                rate = best / CELL_SIZE + (TURN_MAX / d_theta + ACCEL_MAX / d_speed)
                step_buf[...] = CFL_NUMBER / rate
            y_pass(s, h)
            if s < 2:
                def pack(i, carry, s=s, h=h):
                    for j in range(nh):
                        if h == 0:
                            ysend[s + 1, 0, i, pl.ds(3 * j, 3), :] = us[s + 1][i, j, pl.ds(8, 3), :]
                        if h == halves - 1:
                            ysend[s + 1, 1, i, pl.ds(3 * j, 3), :] = us[s + 1][i, j, pl.ds(8 + ny - 3, 3), :]
                    return carry
                lax.fori_loop(0, nx, pack, 0)
                start_half(s + 1, h)
            else:
                copy = pltpu.make_async_copy(
                    out_v.at[:, :, inner(h), :], out_hbm.at[:, :, inner(h), :], out_sem.at[h])
                copy.start()
                out_copies.append(copy)

    for copy in top_copies[0] + top_copies[1]:
        copy.wait_send()
    for s in range(3):
        for h in range(halves):
            down, up = x_copies(s, h)
            pl.when(below_x)(down.wait_send)
            pl.when(above_x)(up.wait_send)
            for copy in h_copies(s, h):
                copy.wait_send()
        down, up = y_copies(s)
        pl.when(below_y)(down.wait_send)
        pl.when(above_y)(up.wait_send)
    for copy in out_copies:
        copy.wait()


def solution(mesh):
    gx_n, gy_n, ha_n = mesh.shape["gx"], mesh.shape["gy"], mesh.shape["ha"]

    def body(level_set, wind_field):
        nx, ny, nh, nv = level_set.shape
        halves = ny // 8
        f32 = jnp.float32
        field = pltpu.VMEM((nx, nh, ny + 16, nv), f32)
        plain = pltpu.VMEM((nx, nh, ny, nv), f32)
        y_rows = -(-3 * nh // 8) * 8
        dma = pltpu.SemaphoreType.DMA
        block = jnp.transpose(level_set, (0, 2, 1, 3))
        out = pl.pallas_call(
            functools.partial(kernel, (gx_n, gy_n, ha_n, nx, nh, ny, nv)),
            out_shape=jax.ShapeDtypeStruct(block.shape, f32),
            in_specs=[
                pl.BlockSpec(memory_space=pl.ANY),
                pl.BlockSpec(memory_space=pltpu.VMEM),
            ],
            out_specs=pl.BlockSpec(memory_space=pl.ANY),
            scratch_shapes=[
                field, field, field,
                plain, plain, plain, plain, plain,
                pltpu.VMEM((3, halves, 3, nh, 8, nv), f32),
                pltpu.VMEM((3, halves, 3, nh, 8, nv), f32),
                pltpu.VMEM((3, halves, nx, 3, 8, nv), f32),
                pltpu.VMEM((3, halves, nx, 3, 8, nv), f32),
                pltpu.VMEM((3, nx, y_rows, nv), f32),
                pltpu.VMEM((3, nx, y_rows, nv), f32),
                pltpu.VMEM((3, 2, nx, y_rows, nv), f32),
                pltpu.VMEM((nh * ha_n, nv), f32),
                pltpu.VMEM((nh * ha_n, nv), f32),
                pltpu.VMEM((nx, ny, nv), f32),
                pltpu.VMEM((nx, ny, nv), f32),
                pltpu.VMEM((8, nv), f32),
                pltpu.VMEM((gx_n - 1, 8, nv), f32),
                pltpu.VMEM((gy_n - 1, 8, nv), f32),
                pltpu.VMEM((2, 8, nv), f32),
                plain,
                dma((1,)), dma((halves,)),
                dma((3, halves, 2)), dma((3, halves, 2)),
                dma((3, halves, 2)), dma((3, halves, 2)),
                dma((3, 2)), dma((3, 2)),
                dma((2, max(gx_n, gy_n))), dma((2, max(gx_n, gy_n))),
            ],
            compiler_params=pltpu.CompilerParams(collective_id=0, has_side_effects=True),
        )(block, wind_field)
        return jnp.transpose(out, (0, 2, 1, 3))

    return jax.shard_map(
        body,
        mesh=mesh,
        in_specs=(P("gx", "gy", "ha", None), P(None, "gx", "gy")),
        out_specs=P("gx", "gy", "ha", None),
        check_vma=False,
    )
```

```python
import functools
import math

import jax
import jax.numpy as jnp
import numpy as np
from jax import lax
from jax.experimental import pallas as pl
from jax.experimental.pallas import tpu as pltpu
from jax.sharding import PartitionSpec as P

CELL_SIZE = 0.05
SPEED_LOW = 0.1
SPEED_SPAN = 0.4
TURN_MAX = 1.0
ACCEL_MAX = 0.05
CFL_NUMBER = 0.5
WENO_EPS = 1e-06
SCALE = 64.0
VMEM_LIMIT = 40 * 2**20
V_APART = 2
MESH = pl.DeviceIdType.MESH


def eps_of(spacing):
    return 0.75 * WENO_EPS * (spacing * SCALE) ** 2


def one_side(b1, b2, b3, t1, t2):
    c1 = 3.0 * b1
    c3 = b3 + b3
    return b2 * (c3 * t1 + c1 * t2) / (b2 * (b3 + c1) + c1 * c3)


def both_sides(p, c, m, ta, tb):
    x = m * ta
    y = p * tb
    twice = 2.0 * (x + y)
    p2 = p + p
    m2 = m + m
    total = p + m
    far = 3.0 * (p2 * m)
    left = c * (twice + y) / (c * (total + p2) + far)
    right = c * (twice + x) / (c * (total + m2) + far)
    return left, right


def along(u, eps):
    n = len(u)
    q = [u[k + 1] - u[k] for k in range(n - 1)]
    d = [q[k + 1] - q[k] for k in range(n - 2)]
    s = [None] + [d[k] - d[k - 1] for k in range(1, n - 2)]
    t = [None] + [s[k + 1] - s[k] for k in range(1, n - 3)]
    z = [1.5 * (e * e) for e in d]
    p, c, m = [None], [None], [None]
    for k in range(1, n - 2):
        v = s[k] * s[k] + eps
        x = 0.75 * (d[k - 1] * d[k])
        w = v - x
        c.append(v + x)
        p.append(w + z[k])
        m.append(w + z[k - 1])
    return d, s, t, p, c, m


def kernel(
    sizes,
    u_hbm,
    wind_hbm,
    out_ref,
    wind,
    us,
    acc,
    fx2,
    fx6,
    fy2,
    fy6,
    xlo,
    xhi,
    hlo,
    hhi,
    ylo,
    yhi,
    ysend,
    cos_t,
    sin_t,
    wx,
    wy,
    step_buf,
    vd,
    vq,
    vs,
    vc,
    vp,
    vm,
    vl,
    vr,
    top_x,
    top_y,
    top_send,
    in_sem,
    x_send,
    x_recv,
    h_send,
    h_recv,
    y_send,
    y_recv,
    top_send_sem,
    top_recv_sem,
):
    gx_n, gy_n, ha_n, nx, nh, ny, nv = sizes
    n_head = nh * ha_n
    d_theta = 2.0 * math.pi / n_head
    d_speed = SPEED_SPAN / nv
    gx, gy, ha = lax.axis_index("gx"), lax.axis_index("gy"), lax.axis_index("ha")
    below_x, above_x = gx > 0, gx < gx_n - 1
    below_y, above_y = gy > 0, gy < gy_n - 1
    h_up, h_down = lax.rem(ha + 1, ha_n), lax.rem(ha + ha_n - 1, ha_n)
    halves = ny // 8

    load_in = pltpu.make_async_copy(u_hbm, acc, in_sem.at[0])
    load_wind = pltpu.make_async_copy(wind_hbm, wind, in_sem.at[1])
    load_wind.start()
    load_in.start()

    barrier = pltpu.get_barrier_semaphore()
    for k in range(1, gx_n):
        pl.semaphore_signal(barrier, inc=1, device_id={"gx": lax.rem(gx + k, gx_n)}, device_id_type=MESH)
    for k in range(1, gy_n):
        pl.semaphore_signal(barrier, inc=1, device_id={"gy": lax.rem(gy + k, gy_n)}, device_id_type=MESH)
    pl.semaphore_signal(barrier, inc=1, device_id={"ha": h_up}, device_id_type=MESH)
    pl.semaphore_signal(barrier, inc=1, device_id={"ha": h_down}, device_id_type=MESH)

    def rows(h):
        return pl.ds(8 + 8 * h, 8)

    def inner(h):
        return pl.ds(8 * h, 8)

    def x_copies(s, h):
        u = us.at[s]
        down = pltpu.make_async_remote_copy(
            src_ref=u.at[pl.ds(0, 3), :, rows(h), :], dst_ref=xhi.at[s, h],
            send_sem=x_send.at[s, h, 0], recv_sem=x_recv.at[s, h, 0],
            device_id={"gx": gx - 1}, device_id_type=MESH)
        up = pltpu.make_async_remote_copy(
            src_ref=u.at[pl.ds(nx - 3, 3), :, rows(h), :], dst_ref=xlo.at[s, h],
            send_sem=x_send.at[s, h, 1], recv_sem=x_recv.at[s, h, 1],
            device_id={"gx": gx + 1}, device_id_type=MESH)
        return down, up

    def h_copies(s, h):
        u = us.at[s]
        down = pltpu.make_async_remote_copy(
            src_ref=u.at[:, pl.ds(0, 3), rows(h), :], dst_ref=hhi.at[s, h],
            send_sem=h_send.at[s, h, 0], recv_sem=h_recv.at[s, h, 0],
            device_id={"ha": h_down}, device_id_type=MESH)
        up = pltpu.make_async_remote_copy(
            src_ref=u.at[:, pl.ds(nh - 3, 3), rows(h), :], dst_ref=hlo.at[s, h],
            send_sem=h_send.at[s, h, 1], recv_sem=h_recv.at[s, h, 1],
            device_id={"ha": h_up}, device_id_type=MESH)
        return down, up

    def y_copies(s):
        down = pltpu.make_async_remote_copy(
            src_ref=ysend.at[s, 0], dst_ref=yhi.at[s],
            send_sem=y_send.at[s, 0], recv_sem=y_recv.at[s, 0],
            device_id={"gy": gy - 1}, device_id_type=MESH)
        up = pltpu.make_async_remote_copy(
            src_ref=ysend.at[s, 1], dst_ref=ylo.at[s],
            send_sem=y_send.at[s, 1], recv_sem=y_recv.at[s, 1],
            device_id={"gy": gy + 1}, device_id_type=MESH)
        return down, up

    def start_half(s, h):
        down, up = x_copies(s, h)
        pl.when(below_x)(down.start)
        pl.when(above_x)(up.start)
        down, up = h_copies(s, h)
        down.start()
        up.start()
        copies = y_copies(s)
        if h == 0:
            pl.when(below_y)(copies[0].start)
        if h == halves - 1:
            pl.when(above_y)(copies[1].start)

    angles = lax.broadcasted_iota(jnp.int32, (n_head, nv), 0).astype(jnp.float32) * d_theta
    cos_t[...] = jnp.cos(angles)
    sin_t[...] = jnp.sin(angles)
    load_wind.wait()
    diagonal = lax.broadcasted_iota(jnp.int32, (ny, ny), 0) == lax.broadcasted_iota(jnp.int32, (ny, ny), 1)
    for i in range(nx):
        for part, out in ((0, wx), (1, wy)):
            row = jnp.broadcast_to(wind[part, pl.ds(i, 1), :], (ny, ny))
            column = jnp.sum(jnp.where(diagonal, row, 0.0), axis=1, keepdims=True)
            out[i] = jnp.broadcast_to(column, (ny, nv))

    low = np.float32(SPEED_LOW) + np.float32(SPEED_SPAN) * np.float32(0.5) / np.float32(nv)
    high = np.float32(SPEED_LOW) + np.float32(SPEED_SPAN) * np.float32(nv - 0.5) / np.float32(nv)
    wind_x, wind_y = wind[0], wind[1]

    def rate_of(k, top):
        c = jnp.broadcast_to(cos_t[pl.ds(k, 1), 0:ny], (nx, ny))
        n = jnp.broadcast_to(sin_t[pl.ds(k, 1), 0:ny], (nx, ny))
        for speed in (float(low), float(high)):
            top = jnp.maximum(top, jnp.abs(speed * c + wind_x) + jnp.abs(speed * n + wind_y))
        return top

    top = lax.fori_loop(0, n_head, rate_of, jnp.zeros((nx, ny), jnp.float32), unroll=4)
    top_send[0] = jnp.full((8, nv), jnp.max(top), jnp.float32)

    speeds = SPEED_LOW + SPEED_SPAN * (
        lax.broadcasted_iota(jnp.int32, (1, nv), 1).astype(jnp.float32) + 0.5) / nv

    def flow_of(j, carry):
        c = speeds * cos_t[pl.ds(ha * nh + j, 1), :]
        n = speeds * sin_t[pl.ds(ha * nh + j, 1), :]
        for i in range(nx):
            f = c + wx[i]
            fx2[i, j] = f * (0.5 / CELL_SIZE)
            fx6[i, j] = jnp.abs(f) * (1.0 / (6.0 * CELL_SIZE))
            f = n + wy[i]
            fy2[i, j] = f * (0.5 / CELL_SIZE)
            fy6[i, j] = jnp.abs(f) * (1.0 / (6.0 * CELL_SIZE))
        return carry

    load_in.wait()

    def pack_y(s, i):
        u = us.at[s]
        for j in range(nh):
            ysend[s, 0, i, pl.ds(3 * j, 3), :] = u[i, j, pl.ds(8, 3), :]
            ysend[s, 1, i, pl.ds(3 * j, 3), :] = u[i, j, pl.ds(8 + ny - 3, 3), :]

    def scale_in(i, carry):
        for j in range(nh):
            us[0, i, j, pl.ds(8, ny), :] = acc[i, j] * SCALE
        return carry

    lax.fori_loop(0, nx, scale_in, 0)

    def pack_all(s):
        def body(i, carry):
            pack_y(s, i)
            return carry
        lax.fori_loop(0, nx, body, 0)

    pack_all(0)

    pl.semaphore_wait(barrier, gx_n - 1 + gy_n - 1 + 2)

    def top_copy(axis, me, size, k, phase):
        buf = (top_x, top_y)[phase]
        return pltpu.make_async_remote_copy(
            src_ref=top_send.at[phase], dst_ref=buf.at[k - 1],
            send_sem=top_send_sem.at[phase, k - 1], recv_sem=top_recv_sem.at[phase, k - 1],
            device_id={axis: lax.rem(me + k, size)}, device_id_type=MESH)

    top_copies = [
        [top_copy("gx", gx, gx_n, k, 0) for k in range(1, gx_n)],
        [top_copy("gy", gy, gy_n, k, 1) for k in range(1, gy_n)],
    ]
    for copy in top_copies[0]:
        copy.start()
    for h in range(halves):
        start_half(0, h)
    lax.fori_loop(0, nh, flow_of, 0)

    def v_pass(s):
        u = us.at[s]
        eps = eps_of(d_speed)
        e2 = eps * eps
        factor = ACCEL_MAX / (6.0 * d_speed)
        blocks = [(i, h) for i in range(nx) for h in range(halves)]
        shape = (nh, 8, nv)
        lane = lax.broadcasted_iota(jnp.int32, (8, nv), 1)
        first = jnp.broadcast_to(lane == 0, shape)
        last = jnp.broadcast_to(lane == nv - 1, shape)

        def level_0(i, h):
            v = u[i, :, rows(h), :]
            a = pltpu.roll(v, nv - 1, 2) - v
            b = v - pltpu.roll(v, 1, 2)
            q1 = jnp.where(last, b, a)
            q0 = jnp.where(first, a, b)
            vq[i, h] = 3.0 * (q0 + q1)
            vd[i, h] = q1 - q0

        def level_1(i, h):
            d = vd[i, h]
            dm = pltpu.roll(d, 1, 2)
            s = d - dm
            c = (s * s + eps) + 0.75 * (d * dm)
            r = 1.5 * s
            p = c + r * d
            m = c - r * dm
            vs[i, h] = s
            vc[i, h] = c * c
            vp[i, h] = p * p
            vm[i, h] = m * m

        def level_2(i, h):
            s = vs[i, h]
            ta = s - pltpu.roll(s, 1, 2)
            tb = pltpu.roll(s, nv - 1, 2) - s
            p = pltpu.roll(vp[i, h], 1, 2)
            m = pltpu.roll(vm[i, h], nv - 1, 2)
            c = vc[i, h]
            left = one_side(jnp.where(first, e2, p), c, m, jnp.where(first, 0.0, ta), tb)
            right = one_side(jnp.where(first, e2, m), c, p, jnp.where(first, 0.0, tb), ta)
            vl[i, h] = left + s
            vr[i, h] = right - s

        def level_3(i, h):
            right = pltpu.roll(vr[i, h], nv - 1, 2)
            d3 = vq[i, h]
            acc[i, :, inner(h), :] = factor * jnp.maximum(d3 + right, vl[i, h] - d3)

        levels = (level_0, level_1, level_2, level_3)
        apart = V_APART
        for step in range(len(blocks) + apart * (len(levels) - 1)):
            for n in reversed(range(len(levels))):
                k = step - apart * n
                if 0 <= k < len(blocks):
                    levels[n](*blocks[k])

    def h_pass(s, h):
        u = us.at[s]
        factor = TURN_MAX / (6.0 * d_theta)

        def body(i, carry):
            cells = [hlo[s, h, i, k] for k in range(3)]
            cells += [u[i, k, rows(h), :] for k in range(nh)]
            cells += [hhi[s, h, i, k] for k in range(3)]
            d, sd, t, p, c, m = along(cells, eps_of(d_theta))
            square = lambda r: [None] + [e * e for e in r[1:]]
            p, c, m = square(p), square(c), square(m)
            sides = {}
            for k in range(2, nh + 3):
                sides[k] = both_sides(p[k - 1], c[k], m[k + 1], t[k - 1], t[k])
            for j in range(nh):
                k = j + 2
                d3 = 3.0 * (cells[j + 4] - cells[j + 2])
                value = jnp.maximum(d3 + (sides[k + 1][1] - sd[k + 1]), (sides[k][0] + sd[k]) - d3)
                acc[i, j, inner(h), :] += factor * value
            return carry

        lax.fori_loop(0, nx, body, 0)

    def x_pass(s, h):
        u = us.at[s]

        def body(j, carry):
            cells = [xlo[s, h, k, j] for k in range(3)]
            cells += [u[k, j, rows(h), :] for k in range(nx)]
            cells += [xhi[s, h, k, j] for k in range(3)]
            d, sd, t, p, c, m = along(cells, eps_of(CELL_SIZE))
            for i in range(nx):
                k = i + 2
                f2 = fx2[i, j, inner(h), :]
                ahead = f2 > 0.0
                b1 = jnp.where(ahead, m[k + 2], p[k - 1])
                b2 = jnp.where(ahead, c[k + 1], c[k])
                b3 = jnp.where(ahead, p[k], m[k + 1])
                t1 = jnp.where(ahead, t[k + 1], t[k - 1])
                dd = d[k] - jnp.where(ahead, d[k + 1], d[k - 1])
                fix = one_side(b1 * b1, b2 * b2, b3 * b3, t1, t[k])
                acc[i, j, inner(h), :] += f2 * (cells[i + 4] - cells[i + 2]) + fx6[i, j, inner(h), :] * (dd + fix)
            return carry

        lax.fori_loop(0, nh, body, 0)

    def y_term(u, i, j, h):
        eps = eps_of(CELL_SIZE)
        f2 = fy2[i, j, inner(h), :]
        ahead = f2 > 0.0
        cells = [u[i, j, pl.ds(8 + 8 * h + r, 8), :] for r in range(-3, 4)]
        q = [cells[k + 1] - cells[k] for k in range(6)]
        d = [q[k + 1] - q[k] for k in range(5)]
        e1 = jnp.where(ahead, d[4], d[0])
        e2 = jnp.where(ahead, d[3], d[1])
        e3 = d[2]
        e4 = jnp.where(ahead, d[1], d[3])
        s1, s2, s3 = e2 - e1, e3 - e2, e4 - e3
        e2k, e3k = 0.75 * e2, 0.75 * e3
        b1 = (s1 * s1 + eps) + e2k * (e2 + s1)
        b2 = (s2 * s2 + eps) + e2k * e3
        b3 = (s3 * s3 + eps) + e3k * (e3 - s3)
        fix = one_side(b1 * b1, b2 * b2, b3 * b3, s2 - s1, s3 - s2)
        return f2 * (cells[4] - cells[2]) + fy6[i, j, inner(h), :] * (s2 + fix)

    def y_pass(s, h):
        u = us.at[s]
        dt = step_buf[...]
        keep = jnp.where(s == 1, 0.75, 0.0)
        take = jnp.where(s == 1, 0.25, 1.0)

        def change(i, j):
            total = acc[i, j, inner(h), :] + y_term(u, i, j, h)
            return u[i, j, rows(h), :] + dt * jnp.minimum(total, 0.0)

        @pl.when(s < 2)
        def _():
            def body(i, carry):
                fresh = [keep * us[0, i, j, rows(h), :] + take * change(i, j) for j in range(nh)]
                for j in range(nh):
                    us[s + 1, i, j, rows(h), :] = fresh[j]
                    if h == 0:
                        ysend[s + 1, 0, i, pl.ds(3 * j, 3), :] = fresh[j][0:3]
                    if h == halves - 1:
                        ysend[s + 1, 1, i, pl.ds(3 * j, 3), :] = fresh[j][5:8]
                return carry

            lax.fori_loop(0, nx, body, 0)
            start_half(s + 1, h)

        @pl.when(s == 2)
        def _():
            def body(i, carry):
                for j in range(nh):
                    out_ref[i, j, inner(h), :] = change(i, j) - us[0, i, j, rows(h), :]
                return carry

            lax.fori_loop(0, nx, body, 0)

    def receive_x(s, h):
        u = us.at[s]
        down, up = x_copies(s, h)
        pl.when(above_x)(down.wait_recv)
        pl.when(below_x)(up.wait_recv)

        @pl.when(jnp.logical_not(below_x))
        def _():
            def body(j, carry):
                edge = u[0, j, rows(h), :]
                slope = edge - u[1, j, rows(h), :]
                for r in (1, 2, 3):
                    xlo[s, h, 3 - r, j] = edge + float(r) * slope
                return carry
            lax.fori_loop(0, nh, body, 0)

        @pl.when(jnp.logical_not(above_x))
        def _():
            def body(j, carry):
                edge = u[nx - 1, j, rows(h), :]
                slope = edge - u[nx - 2, j, rows(h), :]
                for r in (1, 2, 3):
                    xhi[s, h, r - 1, j] = edge + float(r) * slope
                return carry
            lax.fori_loop(0, nh, body, 0)

    def receive_h(s, h):
        for copy in h_copies(s, h):
            copy.wait_recv()

    def receive_y(s, which):
        u = us.at[s]
        copy = y_copies(s)[which]
        there = (above_y, below_y)[which]

        @pl.when(there)
        def _():
            copy.wait_recv()

            def body(i, carry):
                for j in range(nh):
                    if which == 0:
                        u[i, j, pl.ds(8 + ny, 3), :] = yhi[s, i, pl.ds(3 * j, 3), :]
                    else:
                        u[i, j, pl.ds(5, 3), :] = ylo[s, i, pl.ds(3 * j, 3), :]
                return carry
            lax.fori_loop(0, nx, body, 0)

        @pl.when(jnp.logical_not(there))
        def _():
            def body(i, carry):
                for j in range(nh):
                    if which == 0:
                        edge = u[i, j, pl.ds(8 + ny - 1, 1), :]
                        slope = edge - u[i, j, pl.ds(8 + ny - 2, 1), :]
                        for r in (1, 2, 3):
                            u[i, j, pl.ds(8 + ny - 1 + r, 1), :] = edge + float(r) * slope
                    else:
                        edge = u[i, j, pl.ds(8, 1), :]
                        slope = edge - u[i, j, pl.ds(9, 1), :]
                        for r in (1, 2, 3):
                            u[i, j, pl.ds(8 - r, 1), :] = edge + float(r) * slope
                return carry
            lax.fori_loop(0, nx, body, 0)

    def stage(s, carry):
        v_pass(s)

        @pl.when(s == 0)
        def _():
            for copy in top_copies[0]:
                copy.wait_recv()
            best = top_send[0]
            for k in range(1, gx_n):
                best = jnp.maximum(best, top_x[k - 1])
            top_send[1] = best
            for copy in top_copies[1]:
                copy.start()

        for h in range(halves):
            receive_h(s, h)
            h_pass(s, h)
            receive_x(s, h)
            x_pass(s, h)
            if h == 0:
                receive_y(s, 1)

                @pl.when(s == 0)
                def _():
                    for copy in top_copies[1]:
                        copy.wait_recv()
                    best = top_send[1]
                    for k in range(1, gy_n):
                        best = jnp.maximum(best, top_y[k - 1])
                    rate = best / CELL_SIZE + (TURN_MAX / d_theta + ACCEL_MAX / d_speed)
                    step_buf[...] = CFL_NUMBER / rate

            if h == halves - 1:
                receive_y(s, 0)
            y_pass(s, h)
        return carry

    lax.fori_loop(0, 3, stage, 0)

    for copy in top_copies[0] + top_copies[1]:
        copy.wait_send()
    for s in range(3):
        for h in range(halves):
            down, up = x_copies(s, h)
            pl.when(below_x)(down.wait_send)
            pl.when(above_x)(up.wait_send)
            for copy in h_copies(s, h):
                copy.wait_send()
        down, up = y_copies(s)
        pl.when(below_y)(down.wait_send)
        pl.when(above_y)(up.wait_send)


def solution(mesh):
    gx_n, gy_n, ha_n = mesh.shape["gx"], mesh.shape["gy"], mesh.shape["ha"]

    def body(level_set, wind_field):
        nx, ny, nh, nv = level_set.shape
        halves = ny // 8
        f32 = jnp.float32
        plain = pltpu.VMEM((nx, nh, ny, nv), f32)
        y_rows = -(-3 * nh // 8) * 8
        block_8 = pltpu.VMEM((nx, halves, nh, 8, nv), f32)
        dma = pltpu.SemaphoreType.DMA
        block = pltpu.with_memory_space_constraint(jnp.transpose(level_set, (0, 2, 1, 3)), pltpu.HBM)
        wind_field = pltpu.with_memory_space_constraint(wind_field, pltpu.HBM)
        out = pl.pallas_call(
            functools.partial(kernel, (gx_n, gy_n, ha_n, nx, nh, ny, nv)),
            out_shape=jax.ShapeDtypeStruct(block.shape, f32),
            in_specs=[
                pl.BlockSpec(memory_space=pltpu.HBM),
                pl.BlockSpec(memory_space=pltpu.HBM),
            ],
            out_specs=pl.BlockSpec(memory_space=pltpu.VMEM),
            scratch_shapes=[
                pltpu.VMEM((2, nx, ny), f32),
                pltpu.VMEM((3, nx, nh, ny + 16, nv), f32),
                plain, plain, plain, plain, plain,
                pltpu.VMEM((3, halves, 3, nh, 8, nv), f32),
                pltpu.VMEM((3, halves, 3, nh, 8, nv), f32),
                pltpu.VMEM((3, halves, nx, 3, 8, nv), f32),
                pltpu.VMEM((3, halves, nx, 3, 8, nv), f32),
                pltpu.VMEM((3, nx, y_rows, nv), f32),
                pltpu.VMEM((3, nx, y_rows, nv), f32),
                pltpu.VMEM((3, 2, nx, y_rows, nv), f32),
                pltpu.VMEM((nh * ha_n, nv), f32),
                pltpu.VMEM((nh * ha_n, nv), f32),
                pltpu.VMEM((nx, ny, nv), f32),
                pltpu.VMEM((nx, ny, nv), f32),
                pltpu.VMEM((8, nv), f32),
                block_8, block_8, block_8, block_8, block_8, block_8, block_8, block_8,
                pltpu.VMEM((gx_n - 1, 8, nv), f32),
                pltpu.VMEM((gy_n - 1, 8, nv), f32),
                pltpu.VMEM((2, 8, nv), f32),
                dma((2,)),
                dma((3, halves, 2)), dma((3, halves, 2)),
                dma((3, halves, 2)), dma((3, halves, 2)),
                dma((3, 2)), dma((3, 2)),
                dma((2, max(gx_n, gy_n))), dma((2, max(gx_n, gy_n))),
            ],
            compiler_params=pltpu.CompilerParams(
                collective_id=0, has_side_effects=True, vmem_limit_bytes=VMEM_LIMIT),
        )(block, wind_field)
        return jnp.transpose(out * (2.0 / 3.0 / SCALE), (0, 2, 1, 3))

    return jax.shard_map(
        body,
        mesh=mesh,
        in_specs=(P("gx", "gy", "ha", None), P(None, "gx", "gy")),
        out_specs=P("gx", "gy", "ha", None),
        check_vma=False,
    )
```

```python
import functools
import math

import jax
import jax.numpy as jnp
import numpy as np
from jax import lax
from jax.experimental import pallas as pl
from jax.experimental.pallas import tpu as pltpu
from jax.sharding import PartitionSpec as P

CELL_SIZE = 0.05
SPEED_LOW = 0.1
SPEED_SPAN = 0.4
TURN_MAX = 1.0
ACCEL_MAX = 0.05
CFL_NUMBER = 0.5
WENO_EPS = 1e-06
SCALE = 64.0
VMEM_LIMIT = 40 * 2**20
V_ROWS = 2
V_APART = 12
MESH = pl.DeviceIdType.MESH


def eps_of(spacing):
    return 0.75 * WENO_EPS * (spacing * SCALE) ** 2


def one_side(b1, b2, b3, t1, t2):
    c1 = 3.0 * b1
    c3 = b3 + b3
    return b2 * (c3 * t1 + c1 * t2) / (b2 * (b3 + c1) + c1 * c3)


def both_sides(p, c, m, ta, tb):
    x = m * ta
    y = p * tb
    twice = 2.0 * (x + y)
    p2 = p + p
    m2 = m + m
    total = p + m
    far = 3.0 * (p2 * m)
    left = c * (twice + y) / (c * (total + p2) + far)
    right = c * (twice + x) / (c * (total + m2) + far)
    return left, right


def along(u, eps):
    n = len(u)
    q = [u[k + 1] - u[k] for k in range(n - 1)]
    d = [q[k + 1] - q[k] for k in range(n - 2)]
    s = [None] + [d[k] - d[k - 1] for k in range(1, n - 2)]
    t = [None] + [s[k + 1] - s[k] for k in range(1, n - 3)]
    z = [1.5 * (e * e) for e in d]
    p, c, m = [None], [None], [None]
    for k in range(1, n - 2):
        v = s[k] * s[k] + eps
        x = 0.75 * (d[k - 1] * d[k])
        w = v - x
        c.append(v + x)
        p.append(w + z[k])
        m.append(w + z[k - 1])
    return d, s, t, p, c, m


def kernel(
    sizes,
    u_hbm,
    wind_hbm,
    out_ref,
    wind,
    us,
    rate_0,
    acc,
    fx2,
    fx6,
    fy2,
    fy6,
    xlo,
    xhi,
    hlo,
    hhi,
    ylo,
    yhi,
    ysend,
    cos_t,
    sin_t,
    wx,
    wy,
    step_buf,
    vd,
    vq,
    vs,
    vc,
    vp,
    vm,
    vl,
    vr,
    top_x,
    top_y,
    top_send,
    in_sem,
    x_send,
    x_recv,
    h_send,
    h_recv,
    y_send,
    y_recv,
    top_send_sem,
    top_recv_sem,
):
    gx_n, gy_n, ha_n, nx, nh, ny, nv = sizes
    n_head = nh * ha_n
    d_theta = 2.0 * math.pi / n_head
    d_speed = SPEED_SPAN / nv
    gx, gy, ha = lax.axis_index("gx"), lax.axis_index("gy"), lax.axis_index("ha")
    below_x, above_x = gx > 0, gx < gx_n - 1
    below_y, above_y = gy > 0, gy < gy_n - 1
    h_up, h_down = lax.rem(ha + 1, ha_n), lax.rem(ha + ha_n - 1, ha_n)
    halves = ny // 8

    load_in = pltpu.make_async_copy(u_hbm, acc, in_sem.at[0])
    load_wind = pltpu.make_async_copy(wind_hbm, wind, in_sem.at[1])
    load_wind.start()
    load_in.start()

    barrier = pltpu.get_barrier_semaphore()
    for k in range(1, gx_n):
        pl.semaphore_signal(barrier, inc=1, device_id={"gx": lax.rem(gx + k, gx_n)}, device_id_type=MESH)
    for k in range(1, gy_n):
        pl.semaphore_signal(barrier, inc=1, device_id={"gy": lax.rem(gy + k, gy_n)}, device_id_type=MESH)
    pl.semaphore_signal(barrier, inc=1, device_id={"ha": h_up}, device_id_type=MESH)
    pl.semaphore_signal(barrier, inc=1, device_id={"ha": h_down}, device_id_type=MESH)

    def rows(h):
        return pl.ds(8 + 8 * h, 8)

    def inner(h):
        return pl.ds(8 * h, 8)

    def field(s):
        return (us.at[0], rate_0, us.at[2])[s]

    def parity(s):
        return s % 2 if isinstance(s, int) else lax.rem(s, 2)

    def base(s):
        return 0 if s == 1 else 8

    def x_copies(s, h, u=None, start=8):
        u = us.at[0] if u is None else u
        place = pl.ds(start + 8 * h, 8)
        down = pltpu.make_async_remote_copy(
            src_ref=u.at[pl.ds(0, 3), :, place, :], dst_ref=xhi.at[s, h],
            send_sem=x_send.at[h, 0], recv_sem=x_recv.at[parity(s), h, 0],
            device_id={"gx": gx - 1}, device_id_type=MESH)
        up = pltpu.make_async_remote_copy(
            src_ref=u.at[pl.ds(nx - 3, 3), :, place, :], dst_ref=xlo.at[s, h],
            send_sem=x_send.at[h, 1], recv_sem=x_recv.at[parity(s), h, 1],
            device_id={"gx": gx + 1}, device_id_type=MESH)
        return down, up

    def h_copies(s, h, u=None, start=8):
        u = us.at[0] if u is None else u
        place = pl.ds(start + 8 * h, 8)
        down = pltpu.make_async_remote_copy(
            src_ref=u.at[:, pl.ds(0, 3), place, :], dst_ref=hhi.at[s, h],
            send_sem=h_send.at[h, 0], recv_sem=h_recv.at[parity(s), h, 0],
            device_id={"ha": h_down}, device_id_type=MESH)
        up = pltpu.make_async_remote_copy(
            src_ref=u.at[:, pl.ds(nh - 3, 3), place, :], dst_ref=hlo.at[s, h],
            send_sem=h_send.at[h, 1], recv_sem=h_recv.at[parity(s), h, 1],
            device_id={"ha": h_up}, device_id_type=MESH)
        return down, up

    def y_copies(s):
        down = pltpu.make_async_remote_copy(
            src_ref=ysend.at[s, 0], dst_ref=yhi.at[s],
            send_sem=y_send.at[0], recv_sem=y_recv.at[parity(s), 0],
            device_id={"gy": gy - 1}, device_id_type=MESH)
        up = pltpu.make_async_remote_copy(
            src_ref=ysend.at[s, 1], dst_ref=ylo.at[s],
            send_sem=y_send.at[1], recv_sem=y_recv.at[parity(s), 1],
            device_id={"gy": gy + 1}, device_id_type=MESH)
        return down, up

    def x_sent(s, h):
        down, up = x_copies(s, h, field(s), base(s))
        pl.when(below_x)(down.wait_send)
        pl.when(above_x)(up.wait_send)

    def h_sent(s, h):
        for copy in h_copies(s, h, field(s), base(s)):
            copy.wait_send()

    def y_sent(s, which):
        pl.when((below_y, above_y)[which])(y_copies(s)[which].wait_send)

    def start_half(s, h):
        if s > 0:
            x_sent(s - 1, h)
            h_sent(s - 1, h)
        down, up = x_copies(s, h, field(s), base(s))
        pl.when(below_x)(down.start)
        pl.when(above_x)(up.start)
        for copy in h_copies(s, h, field(s), base(s)):
            copy.start()

    def start_y(s, which):
        if s > 0:
            y_sent(s - 1, which)
        pl.when((below_y, above_y)[which])(y_copies(s)[which].start)

    angles = lax.broadcasted_iota(jnp.int32, (n_head, nv), 0).astype(jnp.float32) * d_theta
    cos_t[...] = jnp.cos(angles)
    sin_t[...] = jnp.sin(angles)

    load_in.wait()

    def pack_y(s, i):
        u = us.at[s]
        for j in range(nh):
            ysend[s, 0, i, pl.ds(3 * j, 3), :] = u[i, j, pl.ds(8, 3), :]
            ysend[s, 1, i, pl.ds(3 * j, 3), :] = u[i, j, pl.ds(8 + ny - 3, 3), :]

    def scale_in(i, carry):
        for j in range(nh):
            us[0, i, j, pl.ds(8, ny), :] = acc[i, j] * SCALE
        return carry

    lax.fori_loop(0, nx, scale_in, 0)

    def pack_all(s):
        def body(i, carry):
            pack_y(s, i)
            return carry
        lax.fori_loop(0, nx, body, 0)

    pack_all(0)

    pl.semaphore_wait(barrier, gx_n - 1 + gy_n - 1 + 2)
    start_half(0, 0)
    start_y(0, 0)
    start_y(0, 1)

    low = np.float32(SPEED_LOW) + np.float32(SPEED_SPAN) * np.float32(0.5) / np.float32(nv)
    high = np.float32(SPEED_LOW) + np.float32(SPEED_SPAN) * np.float32(nv - 0.5) / np.float32(nv)
    load_wind.wait()
    wind_x, wind_y = wind[0], wind[1]

    def rate_of(k, top):
        c = jnp.broadcast_to(cos_t[pl.ds(k, 1), 0:ny], (nx, ny))
        n = jnp.broadcast_to(sin_t[pl.ds(k, 1), 0:ny], (nx, ny))
        for speed in (float(low), float(high)):
            top = jnp.maximum(top, jnp.abs(speed * c + wind_x) + jnp.abs(speed * n + wind_y))
        return top

    top = lax.fori_loop(0, n_head, rate_of, jnp.zeros((nx, ny), jnp.float32), unroll=4)
    top_send[0] = jnp.full((8, nv), jnp.max(top), jnp.float32)


    def top_copy(axis, me, size, k, phase):
        buf = (top_x, top_y)[phase]
        return pltpu.make_async_remote_copy(
            src_ref=top_send.at[phase], dst_ref=buf.at[k - 1],
            send_sem=top_send_sem.at[phase], recv_sem=top_recv_sem.at[phase],
            device_id={axis: lax.rem(me + k, size)}, device_id_type=MESH)

    def top_all(phase):
        buf = (top_x, top_y)[phase]
        axis, me, size = (("gx", gx, gx_n), ("gy", gy, gy_n))[phase]
        return pltpu.make_async_remote_copy(
            src_ref=buf, dst_ref=buf, send_sem=top_send_sem.at[phase], recv_sem=top_recv_sem.at[phase],
            device_id={axis: lax.rem(me + 1, size)}, device_id_type=MESH)

    top_copies = [
        [top_copy("gx", gx, gx_n, k, 0) for k in range(1, gx_n)],
        [top_copy("gy", gy, gy_n, k, 1) for k in range(1, gy_n)],
    ]
    for copy in top_copies[0]:
        copy.start()

    diagonal = lax.broadcasted_iota(jnp.int32, (ny, ny), 0) == lax.broadcasted_iota(jnp.int32, (ny, ny), 1)
    for i in range(nx):
        for part, out in ((0, wx), (1, wy)):
            row = jnp.broadcast_to(wind[part, pl.ds(i, 1), :], (ny, ny))
            column = jnp.sum(jnp.where(diagonal, row, 0.0), axis=1, keepdims=True)
            out[i] = jnp.broadcast_to(column, (ny, nv))

    speeds = SPEED_LOW + SPEED_SPAN * (
        lax.broadcasted_iota(jnp.int32, (1, nv), 1).astype(jnp.float32) + 0.5) / nv

    def flow_of(j, carry):
        c = speeds * cos_t[pl.ds(ha * nh + j, 1), :]
        n = speeds * sin_t[pl.ds(ha * nh + j, 1), :]
        for i in range(nx):
            f = c + wx[i]
            fx2[i, j] = f * (0.5 / CELL_SIZE)
            fx6[i, j] = jnp.abs(f) * (1.0 / (6.0 * CELL_SIZE))
            f = n + wy[i]
            fy2[i, j] = f * (0.5 / CELL_SIZE)
            fy6[i, j] = jnp.abs(f) * (1.0 / (6.0 * CELL_SIZE))
        return carry

    lax.fori_loop(0, nh, flow_of, 0)
    step_buf[...] = jnp.ones_like(step_buf)

    def v_pass(s):
        u = us.at[s]
        eps = eps_of(d_speed)
        e2 = eps * eps
        factor = ACCEL_MAX / (6.0 * d_speed)
        blocks = [(i, h, g) for i in range(nx) for h in range(halves) for g in range(nh // V_ROWS)]
        shape = (V_ROWS, 8, nv)
        lane = lax.broadcasted_iota(jnp.int32, (8, nv), 1)
        first = jnp.broadcast_to(lane == 0, shape)
        last = jnp.broadcast_to(lane == nv - 1, shape)

        def level_0(i, h, g):
            part = pl.ds(V_ROWS * g, V_ROWS)
            v = u[i, part, rows(h), :]
            a = pltpu.roll(v, nv - 1, 2) - v
            b = v - pltpu.roll(v, 1, 2)
            q1 = jnp.where(last, b, a)
            q0 = jnp.where(first, a, b)
            vq[i, h, part] = 3.0 * (q0 + q1)
            vd[i, h, part] = q1 - q0

        def level_1(i, h, g):
            part = pl.ds(V_ROWS * g, V_ROWS)
            d = vd[i, h, part]
            dm = pltpu.roll(d, 1, 2)
            s = d - dm
            c = (s * s + eps) + 0.75 * (d * dm)
            r = 1.5 * s
            p = c + r * d
            m = c - r * dm
            vs[i, h, part] = s
            vc[i, h, part] = c * c
            vp[i, h, part] = p * p
            vm[i, h, part] = m * m

        def level_2(i, h, g):
            part = pl.ds(V_ROWS * g, V_ROWS)
            s = vs[i, h, part]
            ta = s - pltpu.roll(s, 1, 2)
            tb = pltpu.roll(s, nv - 1, 2) - s
            p = pltpu.roll(vp[i, h, part], 1, 2)
            m = pltpu.roll(vm[i, h, part], nv - 1, 2)
            c = vc[i, h, part]
            left = one_side(jnp.where(first, e2, p), c, m, jnp.where(first, 0.0, ta), tb)
            right = one_side(jnp.where(first, e2, m), c, p, jnp.where(first, 0.0, tb), ta)
            vl[i, h, part] = left + s
            vr[i, h, part] = right - s

        def level_3(i, h, g):
            part = pl.ds(V_ROWS * g, V_ROWS)
            right = pltpu.roll(vr[i, h, part], nv - 1, 2)
            d3 = vq[i, h, part]
            acc[i, part, inner(h), :] = factor * jnp.maximum(d3 + right, vl[i, h, part] - d3)

        levels = (level_0, level_1, level_2, level_3)
        apart = V_APART
        for step in range(len(blocks) + apart * (len(levels) - 1)):
            for n in reversed(range(len(levels))):
                k = step - apart * n
                if 0 <= k < len(blocks):
                    levels[n](*blocks[k])

    def h_pass(s, h):
        u = us.at[s]
        factor = TURN_MAX / (6.0 * d_theta)

        def body(i, carry):
            cells = [hlo[s, h, i, k] for k in range(3)]
            cells += [u[i, k, rows(h), :] for k in range(nh)]
            cells += [hhi[s, h, i, k] for k in range(3)]
            d, sd, t, p, c, m = along(cells, eps_of(d_theta))
            square = lambda r: [None] + [e * e for e in r[1:]]
            p, c, m = square(p), square(c), square(m)
            sides = {}
            for k in range(2, nh + 3):
                sides[k] = both_sides(p[k - 1], c[k], m[k + 1], t[k - 1], t[k])
            for j in range(nh):
                k = j + 2
                d3 = 3.0 * (cells[j + 4] - cells[j + 2])
                value = jnp.maximum(d3 + (sides[k + 1][1] - sd[k + 1]), (sides[k][0] + sd[k]) - d3)
                acc[i, j, inner(h), :] += factor * value
            return carry

        lax.fori_loop(0, nx, body, 0, unroll=2)

    def x_pass(s, h, store):
        u = us.at[s]

        def body(j, carry):
            cells = [xlo[s, h, k, j] for k in range(3)]
            cells += [u[k, j, rows(h), :] for k in range(nx)]
            cells += [xhi[s, h, k, j] for k in range(3)]
            d, sd, t, p, c, m = along(cells, eps_of(CELL_SIZE))
            for i in range(nx):
                k = i + 2
                f2 = fx2[i, j, inner(h), :]
                ahead = f2 > 0.0
                b1 = jnp.where(ahead, m[k + 2], p[k - 1])
                b2 = jnp.where(ahead, c[k + 1], c[k])
                b3 = jnp.where(ahead, p[k], m[k + 1])
                t1 = jnp.where(ahead, t[k + 1], t[k - 1])
                dd = d[k] - jnp.where(ahead, d[k + 1], d[k - 1])
                fix = one_side(b1 * b1, b2 * b2, b3 * b3, t1, t[k])
                term = f2 * (cells[i + 4] - cells[i + 2]) + fx6[i, j, inner(h), :] * (dd + fix)
                store(i, j, h, acc[i, j, inner(h), :] + term)
            return carry

        lax.fori_loop(0, nh, body, 0, unroll=2)

    def y_term(u, i, j, h):
        eps = eps_of(CELL_SIZE)
        f2 = fy2[i, j, inner(h), :]
        ahead = f2 > 0.0
        cells = [u[i, j, pl.ds(8 + 8 * h + r, 8), :] for r in range(-3, 4)]
        q = [cells[k + 1] - cells[k] for k in range(6)]
        d = [q[k + 1] - q[k] for k in range(5)]
        e1 = jnp.where(ahead, d[4], d[0])
        e2 = jnp.where(ahead, d[3], d[1])
        e3 = d[2]
        e4 = jnp.where(ahead, d[1], d[3])
        s1, s2, s3 = e2 - e1, e3 - e2, e4 - e3
        e2k, e3k = 0.75 * e2, 0.75 * e3
        b1 = (s1 * s1 + eps) + e2k * (e2 + s1)
        b2 = (s2 * s2 + eps) + e2k * e3
        b3 = (s3 * s3 + eps) + e3k * (e3 - s3)
        fix = one_side(b1 * b1, b2 * b2, b3 * b3, s2 - s1, s3 - s2)
        return f2 * (cells[4] - cells[2]) + fy6[i, j, inner(h), :] * (s2 + fix)

    def add_up(i, j, h, total):
        acc[i, j, inner(h), :] = total

    def keep_rate(i, j, h, total):
        rate_0[i, j, inner(h), :] = jnp.minimum(total, 0.0)

    def y_first(h):
        def body(i, carry):
            for j in range(nh):
                acc[i, j, inner(h), :] += y_term(us.at[0], i, j, h)
            return carry

        lax.fori_loop(0, nx, body, 0, unroll=2)

    def pack_first(h):
        def body(i, carry):
            for j in range(nh):
                if h == 0:
                    ysend[1, 0, i, pl.ds(3 * j, 3), :] = rate_0[i, j, 0:3, :]
                if h == halves - 1:
                    ysend[1, 1, i, pl.ds(3 * j, 3), :] = rate_0[i, j, ny - 3:ny, :]
            return carry

        lax.fori_loop(0, nx, body, 0)

    def y_second(h):
        dt = 0.25 * step_buf[...]

        def body(i, carry):
            for j in range(nh):
                change = jnp.minimum(acc[i, j, inner(h), :] + y_term(us.at[1], i, j, h), 0.0)
                fresh = (0.75 * us[0, i, j, rows(h), :] + 0.25 * us[1, i, j, rows(h), :]) + dt * change
                us[2, i, j, rows(h), :] = fresh
                if h == 0:
                    ysend[2, 0, i, pl.ds(3 * j, 3), :] = fresh[0:3]
                if h == halves - 1:
                    ysend[2, 1, i, pl.ds(3 * j, 3), :] = fresh[5:8]
            return carry

        lax.fori_loop(0, nx, body, 0, unroll=2)
        start_half(2, h)
        if h == 0:
            start_y(2, 0)
        if h == halves - 1:
            start_y(2, 1)

    def y_third(h):
        dt = step_buf[...]

        def body(i, carry):
            for j in range(nh):
                change = jnp.minimum(acc[i, j, inner(h), :] + y_term(us.at[2], i, j, h), 0.0)
                out_ref[i, j, inner(h), :] = (us[2, i, j, rows(h), :] - us[0, i, j, rows(h), :]) + dt * change
            return carry

        lax.fori_loop(0, nx, body, 0, unroll=2)

    def receive_x(s, h):
        u = us.at[s]
        down, up = x_copies(s, h)
        pl.when(above_x)(down.wait_recv)
        pl.when(below_x)(up.wait_recv)

        def stepped(halo):
            def body(k, carry):
                dt = step_buf[...]
                for j in range(nh):
                    halo[1, h, k, j] = halo[0, h, k, j] + dt * halo[1, h, k, j]
                return carry
            lax.fori_loop(0, 3, body, 0)

        pl.when(jnp.logical_and(s == 1, above_x))(lambda: stepped(xhi))
        pl.when(jnp.logical_and(s == 1, below_x))(lambda: stepped(xlo))

        @pl.when(jnp.logical_not(below_x))
        def _():
            def body(j, carry):
                edge = u[0, j, rows(h), :]
                slope = edge - u[1, j, rows(h), :]
                for r in (1, 2, 3):
                    xlo[s, h, 3 - r, j] = edge + float(r) * slope
                return carry
            lax.fori_loop(0, nh, body, 0)

        @pl.when(jnp.logical_not(above_x))
        def _():
            def body(j, carry):
                edge = u[nx - 1, j, rows(h), :]
                slope = edge - u[nx - 2, j, rows(h), :]
                for r in (1, 2, 3):
                    xhi[s, h, r - 1, j] = edge + float(r) * slope
                return carry
            lax.fori_loop(0, nh, body, 0)

    def receive_h(s, h):
        for copy in h_copies(s, h):
            copy.wait_recv()

        @pl.when(s == 1)
        def _():
            def body(i, carry):
                dt = step_buf[...]
                for k in range(3):
                    hlo[1, h, i, k] = hlo[0, h, i, k] + dt * hlo[1, h, i, k]
                    hhi[1, h, i, k] = hhi[0, h, i, k] + dt * hhi[1, h, i, k]
                return carry
            lax.fori_loop(0, nx, body, 0)

    def receive_y(s, which):
        u = us.at[s]
        copy = y_copies(s)[which]
        there = (above_y, below_y)[which]

        @pl.when(there)
        def _():
            copy.wait_recv()

            halo = (yhi, ylo)[which]
            place = pl.ds((8 + ny, 5)[which], 3)

            @pl.when(s == 1)
            def _():
                def body(i, carry):
                    halo[1, i] = halo[0, i] + step_buf[0:1, :] * halo[1, i]
                    return carry
                lax.fori_loop(0, nx, body, 0)

            def body(i, carry):
                for j in range(nh):
                    u[i, j, place, :] = halo[s, i, pl.ds(3 * j, 3), :]
                return carry
            lax.fori_loop(0, nx, body, 0)

        @pl.when(jnp.logical_not(there))
        def _():
            def body(i, carry):
                for j in range(nh):
                    if which == 0:
                        edge = u[i, j, pl.ds(8 + ny - 1, 1), :]
                        slope = edge - u[i, j, pl.ds(8 + ny - 2, 1), :]
                        for r in (1, 2, 3):
                            u[i, j, pl.ds(8 + ny - 1 + r, 1), :] = edge + float(r) * slope
                    else:
                        edge = u[i, j, pl.ds(8, 1), :]
                        slope = edge - u[i, j, pl.ds(9, 1), :]
                        for r in (1, 2, 3):
                            u[i, j, pl.ds(8 - r, 1), :] = edge + float(r) * slope
                return carry
            lax.fori_loop(0, nx, body, 0)

    def apply_step():
        top_all(1).wait_recv()
        best = top_send[1]
        for k in range(1, gy_n):
            best = jnp.maximum(best, top_y[k - 1])
        rate = best / CELL_SIZE + (TURN_MAX / d_theta + ACCEL_MAX / d_speed)
        dt = CFL_NUMBER / rate
        step_buf[...] = dt

        def body(i, carry):
            fresh = [us[0, i, j, rows(h), :] + dt * rate_0[i, j, inner(h), :] for j in range(nh) for h in range(halves)]
            for j in range(nh):
                for h in range(halves):
                    us[1, i, j, rows(h), :] = fresh[j * halves + h]
            return carry

        lax.fori_loop(0, nx, body, 0)

    def first_stage():
        for h in range(1, halves):
            start_half(0, h)
        receive_y(0, 0)
        receive_y(0, 1)
        for h in range(halves):
            y_first(h)
            receive_h(0, h)
            h_pass(0, h)
            receive_x(0, h)
            x_pass(0, h, keep_rate)
            pack_first(h)
            start_half(1, h)
            if h == 0:
                start_y(1, 0)
                top_all(0).wait_recv()
                best = top_send[0]
                for k in range(1, gx_n):
                    best = jnp.maximum(best, top_x[k - 1])
                top_send[1] = best
                for copy in top_copies[1]:
                    copy.start()
            if h == halves - 1:
                start_y(1, 1)

    def later_stage(s):
        for h in range(halves):
            receive_h(s, h)
            h_pass(s, h)
            receive_x(s, h)
            x_pass(s, h, add_up)
            if h == 0:
                receive_y(s, 1)
            if h == halves - 1:
                receive_y(s, 0)
            pl.when(s == 1)(lambda: y_second(h))
            pl.when(s == 2)(lambda: y_third(h))

    def stage(s, carry):
        pl.when(s == 1)(apply_step)
        v_pass(s)
        pl.when(s == 0)(first_stage)
        pl.when(s > 0)(lambda: later_stage(s))
        return carry

    lax.fori_loop(0, 3, stage, 0)

    top_all(0).wait_send()
    top_all(1).wait_send()
    for h in range(halves):
        x_sent(2, h)
        h_sent(2, h)
    y_sent(2, 0)
    y_sent(2, 1)


def solution(mesh):
    gx_n, gy_n, ha_n = mesh.shape["gx"], mesh.shape["gy"], mesh.shape["ha"]

    def body(level_set, wind_field):
        nx, ny, nh, nv = level_set.shape
        halves = ny // 8
        f32 = jnp.float32
        plain = pltpu.VMEM((nx, nh, ny, nv), f32)
        y_rows = -(-3 * nh // 8) * 8
        block_8 = pltpu.VMEM((nx, halves, nh, 8, nv), f32)
        dma = pltpu.SemaphoreType.DMA
        block = pltpu.with_memory_space_constraint(jnp.transpose(level_set, (0, 2, 1, 3)), pltpu.HBM)
        wind_field = pltpu.with_memory_space_constraint(wind_field, pltpu.HBM)
        out = pl.pallas_call(
            functools.partial(kernel, (gx_n, gy_n, ha_n, nx, nh, ny, nv)),
            out_shape=jax.ShapeDtypeStruct(block.shape, f32),
            in_specs=[
                pl.BlockSpec(memory_space=pltpu.HBM),
                pl.BlockSpec(memory_space=pltpu.HBM),
            ],
            out_specs=pl.BlockSpec(memory_space=pltpu.VMEM),
            scratch_shapes=[
                pltpu.VMEM((2, nx, ny), f32),
                pltpu.VMEM((3, nx, nh, ny + 16, nv), f32),
                plain,
                plain, plain, plain, plain, plain,
                pltpu.VMEM((3, halves, 3, nh, 8, nv), f32),
                pltpu.VMEM((3, halves, 3, nh, 8, nv), f32),
                pltpu.VMEM((3, halves, nx, 3, 8, nv), f32),
                pltpu.VMEM((3, halves, nx, 3, 8, nv), f32),
                pltpu.VMEM((3, nx, y_rows, nv), f32),
                pltpu.VMEM((3, nx, y_rows, nv), f32),
                pltpu.VMEM((3, 2, nx, y_rows, nv), f32),
                pltpu.VMEM((nh * ha_n, nv), f32),
                pltpu.VMEM((nh * ha_n, nv), f32),
                pltpu.VMEM((nx, ny, nv), f32),
                pltpu.VMEM((nx, ny, nv), f32),
                pltpu.VMEM((8, nv), f32),
                block_8, block_8, block_8, block_8, block_8, block_8, block_8, block_8,
                pltpu.VMEM((gx_n - 1, 8, nv), f32),
                pltpu.VMEM((gy_n - 1, 8, nv), f32),
                pltpu.VMEM((2, 8, nv), f32),
                dma((2,)),
                dma((halves, 2)), dma((2, halves, 2)),
                dma((halves, 2)), dma((2, halves, 2)),
                dma((2,)), dma((2, 2)),
                dma((2,)), dma((2,)),
            ],
            compiler_params=pltpu.CompilerParams(
                collective_id=0, has_side_effects=True, vmem_limit_bytes=VMEM_LIMIT),
        )(block, wind_field)
        return jnp.transpose(out * (2.0 / 3.0 / SCALE), (0, 2, 1, 3))

    return jax.shard_map(
        body,
        mesh=mesh,
        in_specs=(P("gx", "gy", "ha", None), P(None, "gx", "gy")),
        out_specs=P("gx", "gy", "ha", None),
        check_vma=False,
    )
```

```python
import functools
import math

import jax
import jax.numpy as jnp
import numpy as np
from jax import lax
from jax.experimental import pallas as pl
from jax.experimental.pallas import tpu as pltpu
from jax.sharding import PartitionSpec as P

CELL_SIZE = 0.05
SPEED_LOW = 0.1
SPEED_SPAN = 0.4
TURN_MAX = 1.0
ACCEL_MAX = 0.05
CFL_NUMBER = 0.5
WENO_EPS = 1e-06
SCALE = 64.0
VMEM_LIMIT = 40 * 2**20
V_ROWS = 2
V_APART = 12
MESH = pl.DeviceIdType.MESH


def eps_of(spacing):
    return 0.75 * WENO_EPS * (spacing * SCALE) ** 2


def one_side(b1, b2, b3, t1, t2):
    c1 = 3.0 * b1
    c3 = b3 + b3
    return b2 * (c3 * t1 + c1 * t2) / (b2 * (b3 + c1) + c1 * c3)


def both_sides(p, c, m, ta, tb):
    x = m * ta
    y = p * tb
    twice = 2.0 * (x + y)
    p2 = p + p
    m2 = m + m
    total = p + m
    far = 3.0 * (p2 * m)
    left = c * (twice + y) / (c * (total + p2) + far)
    right = c * (twice + x) / (c * (total + m2) + far)
    return left, right


def along(u, eps):
    n = len(u)
    q = [u[k + 1] - u[k] for k in range(n - 1)]
    d = [q[k + 1] - q[k] for k in range(n - 2)]
    s = [None] + [d[k] - d[k - 1] for k in range(1, n - 2)]
    t = [None] + [s[k + 1] - s[k] for k in range(1, n - 3)]
    z = [1.5 * (e * e) for e in d]
    p, c, m = [None], [None], [None]
    for k in range(1, n - 2):
        v = s[k] * s[k] + eps
        x = 0.75 * (d[k - 1] * d[k])
        w = v - x
        c.append(v + x)
        p.append(w + z[k])
        m.append(w + z[k - 1])
    return d, s, t, p, c, m


def kernel(
    sizes,
    u_hbm,
    wind_hbm,
    out_ref,
    wind,
    us,
    rate_0,
    acc,
    fx2,
    fx6,
    fy2,
    fy6,
    xlo,
    xhi,
    hlo,
    hhi,
    ylo,
    yhi,
    ysend,
    cos_t,
    sin_t,
    wx,
    wy,
    step_buf,
    vd,
    vq,
    vs,
    vc,
    vp,
    vm,
    vl,
    vr,
    top_x,
    top_y,
    top_send,
    in_sem,
    x_send,
    x_recv,
    h_send,
    h_recv,
    y_send,
    y_recv,
    top_send_sem,
    top_recv_sem,
):
    gx_n, gy_n, ha_n, nx, nh, ny, nv = sizes
    n_head = nh * ha_n
    d_theta = 2.0 * math.pi / n_head
    d_speed = SPEED_SPAN / nv
    gx, gy, ha = lax.axis_index("gx"), lax.axis_index("gy"), lax.axis_index("ha")
    below_x, above_x = gx > 0, gx < gx_n - 1
    below_y, above_y = gy > 0, gy < gy_n - 1
    h_up, h_down = lax.rem(ha + 1, ha_n), lax.rem(ha + ha_n - 1, ha_n)
    halves = ny // 8

    load_in = pltpu.make_async_copy(u_hbm, acc, in_sem.at[0])
    load_wind = pltpu.make_async_copy(wind_hbm, wind, in_sem.at[1])
    load_wind.start()
    load_in.start()

    barrier = pltpu.get_barrier_semaphore()
    for k in range(1, gx_n):
        pl.semaphore_signal(barrier, inc=1, device_id={"gx": lax.rem(gx + k, gx_n)}, device_id_type=MESH)
    for k in range(1, gy_n):
        pl.semaphore_signal(barrier, inc=1, device_id={"gy": lax.rem(gy + k, gy_n)}, device_id_type=MESH)
    pl.semaphore_signal(barrier, inc=1, device_id={"ha": h_up}, device_id_type=MESH)
    pl.semaphore_signal(barrier, inc=1, device_id={"ha": h_down}, device_id_type=MESH)

    def rows(h):
        return pl.ds(8 + 8 * h, 8)

    def inner(h):
        return pl.ds(8 * h, 8)

    def field(s):
        return (us.at[0], rate_0, us.at[2])[s]

    def parity(s):
        return s % 2 if isinstance(s, int) else lax.rem(s, 2)

    def base(s):
        return 0 if s == 1 else 8

    def x_copies(s, h, u=None, start=8):
        u = us.at[0] if u is None else u
        place = pl.ds(start + 8 * h, 8)
        down = pltpu.make_async_remote_copy(
            src_ref=u.at[pl.ds(0, 3), :, place, :], dst_ref=xhi.at[s, h],
            send_sem=x_send.at[h, 0], recv_sem=x_recv.at[parity(s), h, 0],
            device_id={"gx": gx - 1}, device_id_type=MESH)
        up = pltpu.make_async_remote_copy(
            src_ref=u.at[pl.ds(nx - 3, 3), :, place, :], dst_ref=xlo.at[s, h],
            send_sem=x_send.at[h, 1], recv_sem=x_recv.at[parity(s), h, 1],
            device_id={"gx": gx + 1}, device_id_type=MESH)
        return down, up

    def h_copies(s, h, g, u=None, start=8):
        u = us.at[0] if u is None else u
        place = pl.ds(start + 8 * h, 8)
        layers = pl.ds(g * (nx // 2), nx // 2)
        down = pltpu.make_async_remote_copy(
            src_ref=u.at[layers, pl.ds(0, 3), place, :], dst_ref=hhi.at[s, h, layers],
            send_sem=h_send.at[h, g, 0], recv_sem=h_recv.at[parity(s), h, g, 0],
            device_id={"ha": h_down}, device_id_type=MESH)
        up = pltpu.make_async_remote_copy(
            src_ref=u.at[layers, pl.ds(nh - 3, 3), place, :], dst_ref=hlo.at[s, h, layers],
            send_sem=h_send.at[h, g, 1], recv_sem=h_recv.at[parity(s), h, g, 1],
            device_id={"ha": h_up}, device_id_type=MESH)
        return down, up

    def y_copies(s):
        down = pltpu.make_async_remote_copy(
            src_ref=ysend.at[s, 0], dst_ref=yhi.at[s],
            send_sem=y_send.at[0], recv_sem=y_recv.at[parity(s), 0],
            device_id={"gy": gy - 1}, device_id_type=MESH)
        up = pltpu.make_async_remote_copy(
            src_ref=ysend.at[s, 1], dst_ref=ylo.at[s],
            send_sem=y_send.at[1], recv_sem=y_recv.at[parity(s), 1],
            device_id={"gy": gy + 1}, device_id_type=MESH)
        return down, up

    def x_sent(s, h):
        down, up = x_copies(s, h, field(s), base(s))
        pl.when(below_x)(down.wait_send)
        pl.when(above_x)(up.wait_send)

    def h_sent(s, h):
        for g in range(2):
            for copy in h_copies(s, h, g, field(s), base(s)):
                copy.wait_send()

    def y_sent(s, which):
        pl.when((below_y, above_y)[which])(y_copies(s)[which].wait_send)

    def start_half(s, h):
        if s > 0:
            x_sent(s - 1, h)
            h_sent(s - 1, h)
        for g in range(2):
            for copy in h_copies(s, h, g, field(s), base(s)):
                copy.start()
        down, up = x_copies(s, h, field(s), base(s))
        pl.when(below_x)(down.start)
        pl.when(above_x)(up.start)

    def start_y(s, which):
        if s > 0:
            y_sent(s - 1, which)
        pl.when((below_y, above_y)[which])(y_copies(s)[which].start)

    angles = lax.broadcasted_iota(jnp.int32, (n_head, nv), 0).astype(jnp.float32) * d_theta
    cos_t[...] = jnp.cos(angles)
    sin_t[...] = jnp.sin(angles)

    low = np.float32(SPEED_LOW) + np.float32(SPEED_SPAN) * np.float32(0.5) / np.float32(nv)
    high = np.float32(SPEED_LOW) + np.float32(SPEED_SPAN) * np.float32(nv - 0.5) / np.float32(nv)
    load_wind.wait()
    wind_x, wind_y = wind[0], wind[1]

    def rate_of(k, top):
        c = jnp.broadcast_to(cos_t[pl.ds(k, 1), 0:ny], (nx, ny))
        n = jnp.broadcast_to(sin_t[pl.ds(k, 1), 0:ny], (nx, ny))
        for speed in (float(low), float(high)):
            top = jnp.maximum(top, jnp.abs(speed * c + wind_x) + jnp.abs(speed * n + wind_y))
        return top

    top = lax.fori_loop(0, n_head, rate_of, jnp.zeros((nx, ny), jnp.float32), unroll=4)
    top_send[0] = jnp.full((8, nv), jnp.max(top), jnp.float32)


    def top_copy(axis, me, size, k, phase):
        buf = (top_x, top_y)[phase]
        return pltpu.make_async_remote_copy(
            src_ref=top_send.at[phase], dst_ref=buf.at[k - 1],
            send_sem=top_send_sem.at[phase], recv_sem=top_recv_sem.at[phase],
            device_id={axis: lax.rem(me + k, size)}, device_id_type=MESH)

    def top_all(phase):
        buf = (top_x, top_y)[phase]
        axis, me, size = (("gx", gx, gx_n), ("gy", gy, gy_n))[phase]
        return pltpu.make_async_remote_copy(
            src_ref=buf, dst_ref=buf, send_sem=top_send_sem.at[phase], recv_sem=top_recv_sem.at[phase],
            device_id={axis: lax.rem(me + 1, size)}, device_id_type=MESH)

    top_copies = [
        [top_copy("gx", gx, gx_n, k, 0) for k in range(1, gx_n)],
        [top_copy("gy", gy, gy_n, k, 1) for k in range(1, gy_n)],
    ]
    load_in.wait()

    def pack_y(s, i):
        u = us.at[s]
        for j in range(nh):
            ysend[s, 0, i, pl.ds(3 * j, 3), :] = u[i, j, pl.ds(8, 3), :]
            ysend[s, 1, i, pl.ds(3 * j, 3), :] = u[i, j, pl.ds(8 + ny - 3, 3), :]

    def scale_in(i, carry):
        for j in range(nh):
            us[0, i, j, pl.ds(8, ny), :] = acc[i, j] * SCALE
        return carry

    lax.fori_loop(0, nx, scale_in, 0)

    def pack_all(s):
        def body(i, carry):
            pack_y(s, i)
            return carry
        lax.fori_loop(0, nx, body, 0)

    pack_all(0)

    pl.semaphore_wait(barrier, gx_n - 1 + gy_n - 1 + 2)
    for copy in top_copies[0]:
        copy.start()
    start_half(0, 0)
    start_y(0, 0)
    start_y(0, 1)


    diagonal = lax.broadcasted_iota(jnp.int32, (ny, ny), 0) == lax.broadcasted_iota(jnp.int32, (ny, ny), 1)
    for i in range(nx):
        for part, out in ((0, wx), (1, wy)):
            row = jnp.broadcast_to(wind[part, pl.ds(i, 1), :], (ny, ny))
            column = jnp.sum(jnp.where(diagonal, row, 0.0), axis=1, keepdims=True)
            out[i] = jnp.broadcast_to(column, (ny, nv))

    speeds = SPEED_LOW + SPEED_SPAN * (
        lax.broadcasted_iota(jnp.int32, (1, nv), 1).astype(jnp.float32) + 0.5) / nv

    def flow_of(j, carry):
        c = speeds * cos_t[pl.ds(ha * nh + j, 1), :]
        n = speeds * sin_t[pl.ds(ha * nh + j, 1), :]
        for i in range(nx):
            f = c + wx[i]
            fx2[i, j] = f * (0.5 / CELL_SIZE)
            fx6[i, j] = jnp.abs(f) * (1.0 / (6.0 * CELL_SIZE))
            f = n + wy[i]
            fy2[i, j] = f * (0.5 / CELL_SIZE)
            fy6[i, j] = jnp.abs(f) * (1.0 / (6.0 * CELL_SIZE))
        return carry

    lax.fori_loop(0, nh, flow_of, 0)
    step_buf[...] = jnp.ones_like(step_buf)

    def v_pass(s):
        u = us.at[s]
        eps = eps_of(d_speed)
        e2 = eps * eps
        factor = ACCEL_MAX / (6.0 * d_speed)
        blocks = [(i, h, g) for i in range(nx) for h in range(halves) for g in range(nh // V_ROWS)]
        shape = (V_ROWS, 8, nv)
        lane = lax.broadcasted_iota(jnp.int32, (8, nv), 1)
        first = jnp.broadcast_to(lane == 0, shape)
        last = jnp.broadcast_to(lane == nv - 1, shape)

        def level_0(i, h, g):
            part = pl.ds(V_ROWS * g, V_ROWS)
            v = u[i, part, rows(h), :]
            a = pltpu.roll(v, nv - 1, 2) - v
            b = v - pltpu.roll(v, 1, 2)
            q1 = jnp.where(last, b, a)
            q0 = jnp.where(first, a, b)
            vq[i, h, part] = 3.0 * (q0 + q1)
            vd[i, h, part] = q1 - q0

        def level_1(i, h, g):
            part = pl.ds(V_ROWS * g, V_ROWS)
            d = vd[i, h, part]
            dm = pltpu.roll(d, 1, 2)
            s = d - dm
            c = (s * s + eps) + 0.75 * (d * dm)
            r = 1.5 * s
            p = c + r * d
            m = c - r * dm
            vs[i, h, part] = s
            vc[i, h, part] = c * c
            vp[i, h, part] = p * p
            vm[i, h, part] = m * m

        def level_2(i, h, g):
            part = pl.ds(V_ROWS * g, V_ROWS)
            s = vs[i, h, part]
            ta = s - pltpu.roll(s, 1, 2)
            tb = pltpu.roll(s, nv - 1, 2) - s
            p = pltpu.roll(vp[i, h, part], 1, 2)
            m = pltpu.roll(vm[i, h, part], nv - 1, 2)
            c = vc[i, h, part]
            left = one_side(jnp.where(first, e2, p), c, m, jnp.where(first, 0.0, ta), tb)
            right = one_side(jnp.where(first, e2, m), c, p, jnp.where(first, 0.0, tb), ta)
            vl[i, h, part] = left + s
            vr[i, h, part] = right - s

        def level_3(i, h, g):
            part = pl.ds(V_ROWS * g, V_ROWS)
            right = pltpu.roll(vr[i, h, part], nv - 1, 2)
            d3 = vq[i, h, part]
            acc[i, part, inner(h), :] = factor * jnp.maximum(d3 + right, vl[i, h, part] - d3)

        levels = (level_0, level_1, level_2, level_3)
        apart = V_APART
        for step in range(len(blocks) + apart * (len(levels) - 1)):
            for n in reversed(range(len(levels))):
                k = step - apart * n
                if 0 <= k < len(blocks):
                    levels[n](*blocks[k])

    def h_pass(s, h, g):
        u = us.at[s]
        factor = TURN_MAX / (6.0 * d_theta)

        def body(i, carry):
            cells = [hlo[s, h, i, k] for k in range(3)]
            cells += [u[i, k, rows(h), :] for k in range(nh)]
            cells += [hhi[s, h, i, k] for k in range(3)]
            d, sd, t, p, c, m = along(cells, eps_of(d_theta))
            square = lambda r: [None] + [e * e for e in r[1:]]
            p, c, m = square(p), square(c), square(m)
            sides = {}
            for k in range(2, nh + 3):
                sides[k] = both_sides(p[k - 1], c[k], m[k + 1], t[k - 1], t[k])
            for j in range(nh):
                k = j + 2
                d3 = 3.0 * (cells[j + 4] - cells[j + 2])
                value = jnp.maximum(d3 + (sides[k + 1][1] - sd[k + 1]), (sides[k][0] + sd[k]) - d3)
                acc[i, j, inner(h), :] += factor * value
            return carry

        lax.fori_loop(g * (nx // 2), (g + 1) * (nx // 2), body, 0, unroll=2)

    def x_pass(s, h, store):
        u = us.at[s]

        def body(j, carry):
            cells = [xlo[s, h, k, j] for k in range(3)]
            cells += [u[k, j, rows(h), :] for k in range(nx)]
            cells += [xhi[s, h, k, j] for k in range(3)]
            d, sd, t, p, c, m = along(cells, eps_of(CELL_SIZE))
            for i in range(nx):
                k = i + 2
                f2 = fx2[i, j, inner(h), :]
                ahead = f2 > 0.0
                b1 = jnp.where(ahead, m[k + 2], p[k - 1])
                b2 = jnp.where(ahead, c[k + 1], c[k])
                b3 = jnp.where(ahead, p[k], m[k + 1])
                t1 = jnp.where(ahead, t[k + 1], t[k - 1])
                dd = d[k] - jnp.where(ahead, d[k + 1], d[k - 1])
                fix = one_side(b1 * b1, b2 * b2, b3 * b3, t1, t[k])
                term = f2 * (cells[i + 4] - cells[i + 2]) + fx6[i, j, inner(h), :] * (dd + fix)
                store(i, j, h, acc[i, j, inner(h), :] + term)
            return carry

        lax.fori_loop(0, nh, body, 0, unroll=2)

    def y_term(u, i, j, h):
        eps = eps_of(CELL_SIZE)
        f2 = fy2[i, j, inner(h), :]
        ahead = f2 > 0.0
        cells = [u[i, j, pl.ds(8 + 8 * h + r, 8), :] for r in range(-3, 4)]
        q = [cells[k + 1] - cells[k] for k in range(6)]
        d = [q[k + 1] - q[k] for k in range(5)]
        e1 = jnp.where(ahead, d[4], d[0])
        e2 = jnp.where(ahead, d[3], d[1])
        e3 = d[2]
        e4 = jnp.where(ahead, d[1], d[3])
        s1, s2, s3 = e2 - e1, e3 - e2, e4 - e3
        e2k, e3k = 0.75 * e2, 0.75 * e3
        b1 = (s1 * s1 + eps) + e2k * (e2 + s1)
        b2 = (s2 * s2 + eps) + e2k * e3
        b3 = (s3 * s3 + eps) + e3k * (e3 - s3)
        fix = one_side(b1 * b1, b2 * b2, b3 * b3, s2 - s1, s3 - s2)
        return f2 * (cells[4] - cells[2]) + fy6[i, j, inner(h), :] * (s2 + fix)

    def add_up(i, j, h, total):
        acc[i, j, inner(h), :] = total

    def keep_rate(i, j, h, total):
        rate_0[i, j, inner(h), :] = jnp.minimum(total, 0.0)

    def y_first(h):
        def body(i, carry):
            for j in range(nh):
                acc[i, j, inner(h), :] += y_term(us.at[0], i, j, h)
            return carry

        lax.fori_loop(0, nx, body, 0, unroll=2)

    def pack_first(h):
        def body(i, carry):
            for j in range(nh):
                if h == 0:
                    ysend[1, 0, i, pl.ds(3 * j, 3), :] = rate_0[i, j, 0:3, :]
                if h == halves - 1:
                    ysend[1, 1, i, pl.ds(3 * j, 3), :] = rate_0[i, j, ny - 3:ny, :]
            return carry

        lax.fori_loop(0, nx, body, 0)

    def y_second(h):
        dt = 0.25 * step_buf[...]

        def body(i, carry):
            for j in range(nh):
                change = jnp.minimum(acc[i, j, inner(h), :] + y_term(us.at[1], i, j, h), 0.0)
                fresh = (0.75 * us[0, i, j, rows(h), :] + 0.25 * us[1, i, j, rows(h), :]) + dt * change
                us[2, i, j, rows(h), :] = fresh
                if h == 0:
                    ysend[2, 0, i, pl.ds(3 * j, 3), :] = fresh[0:3]
                if h == halves - 1:
                    ysend[2, 1, i, pl.ds(3 * j, 3), :] = fresh[5:8]
            return carry

        lax.fori_loop(0, nx, body, 0, unroll=2)
        start_half(2, h)
        if h == 0:
            start_y(2, 0)
        if h == halves - 1:
            start_y(2, 1)

    def y_third(h):
        dt = step_buf[...]

        def body(i, carry):
            for j in range(nh):
                change = jnp.minimum(acc[i, j, inner(h), :] + y_term(us.at[2], i, j, h), 0.0)
                out_ref[i, j, inner(h), :] = (us[2, i, j, rows(h), :] - us[0, i, j, rows(h), :]) + dt * change
            return carry

        lax.fori_loop(0, nx, body, 0, unroll=2)

    def receive_x(s, h):
        u = us.at[s]
        down, up = x_copies(s, h)
        pl.when(above_x)(down.wait_recv)
        pl.when(below_x)(up.wait_recv)

        def stepped(halo):
            def body(k, carry):
                dt = step_buf[...]
                for j in range(nh):
                    halo[1, h, k, j] = halo[0, h, k, j] + dt * halo[1, h, k, j]
                return carry
            lax.fori_loop(0, 3, body, 0)

        pl.when(jnp.logical_and(s == 1, above_x))(lambda: stepped(xhi))
        pl.when(jnp.logical_and(s == 1, below_x))(lambda: stepped(xlo))

        @pl.when(jnp.logical_not(below_x))
        def _():
            def body(j, carry):
                edge = u[0, j, rows(h), :]
                slope = edge - u[1, j, rows(h), :]
                for r in (1, 2, 3):
                    xlo[s, h, 3 - r, j] = edge + float(r) * slope
                return carry
            lax.fori_loop(0, nh, body, 0)

        @pl.when(jnp.logical_not(above_x))
        def _():
            def body(j, carry):
                edge = u[nx - 1, j, rows(h), :]
                slope = edge - u[nx - 2, j, rows(h), :]
                for r in (1, 2, 3):
                    xhi[s, h, r - 1, j] = edge + float(r) * slope
                return carry
            lax.fori_loop(0, nh, body, 0)

    def receive_h(s, h, g):
        for copy in h_copies(s, h, g):
            copy.wait_recv()

        @pl.when(s == 1)
        def _():
            def body(i, carry):
                dt = step_buf[...]
                for k in range(3):
                    hlo[1, h, i, k] = hlo[0, h, i, k] + dt * hlo[1, h, i, k]
                    hhi[1, h, i, k] = hhi[0, h, i, k] + dt * hhi[1, h, i, k]
                return carry
            lax.fori_loop(g * (nx // 2), (g + 1) * (nx // 2), body, 0)

    def receive_y(s, which):
        u = us.at[s]
        copy = y_copies(s)[which]
        there = (above_y, below_y)[which]

        @pl.when(there)
        def _():
            copy.wait_recv()

            halo = (yhi, ylo)[which]
            place = pl.ds((8 + ny, 5)[which], 3)

            @pl.when(s == 1)
            def _():
                def body(i, carry):
                    halo[1, i] = halo[0, i] + step_buf[0:1, :] * halo[1, i]
                    return carry
                lax.fori_loop(0, nx, body, 0)

            def body(i, carry):
                for j in range(nh):
                    u[i, j, place, :] = halo[s, i, pl.ds(3 * j, 3), :]
                return carry
            lax.fori_loop(0, nx, body, 0)

        @pl.when(jnp.logical_not(there))
        def _():
            def body(i, carry):
                for j in range(nh):
                    if which == 0:
                        edge = u[i, j, pl.ds(8 + ny - 1, 1), :]
                        slope = edge - u[i, j, pl.ds(8 + ny - 2, 1), :]
                        for r in (1, 2, 3):
                            u[i, j, pl.ds(8 + ny - 1 + r, 1), :] = edge + float(r) * slope
                    else:
                        edge = u[i, j, pl.ds(8, 1), :]
                        slope = edge - u[i, j, pl.ds(9, 1), :]
                        for r in (1, 2, 3):
                            u[i, j, pl.ds(8 - r, 1), :] = edge + float(r) * slope
                return carry
            lax.fori_loop(0, nx, body, 0)

    def apply_step():
        top_all(1).wait_recv()
        best = top_send[1]
        for k in range(1, gy_n):
            best = jnp.maximum(best, top_y[k - 1])
        rate = best / CELL_SIZE + (TURN_MAX / d_theta + ACCEL_MAX / d_speed)
        dt = CFL_NUMBER / rate
        step_buf[...] = dt

        def body(i, carry):
            fresh = [us[0, i, j, rows(h), :] + dt * rate_0[i, j, inner(h), :] for j in range(nh) for h in range(halves)]
            for j in range(nh):
                for h in range(halves):
                    us[1, i, j, rows(h), :] = fresh[j * halves + h]
            return carry

        lax.fori_loop(0, nx, body, 0)

    def first_stage():
        for h in range(1, halves):
            start_half(0, h)
        receive_y(0, 0)
        receive_y(0, 1)
        top_all(0).wait_recv()
        best = top_send[0]
        for k in range(1, gx_n):
            best = jnp.maximum(best, top_x[k - 1])
        top_send[1] = best
        for copy in top_copies[1]:
            copy.start()
        for h in range(halves):
            y_first(h)
            for g in range(2):
                receive_h(0, h, g)
                h_pass(0, h, g)
            receive_x(0, h)
            x_pass(0, h, keep_rate)
            pack_first(h)
            start_half(1, h)
            if h == 0:
                start_y(1, 0)
            if h == halves - 1:
                start_y(1, 1)

    def later_stage(s):
        for h in range(halves):
            for g in range(2):
                receive_h(s, h, g)
                h_pass(s, h, g)
            receive_x(s, h)
            x_pass(s, h, add_up)
            if h == 0:
                receive_y(s, 1)
            if h == halves - 1:
                receive_y(s, 0)
            pl.when(s == 1)(lambda: y_second(h))
            pl.when(s == 2)(lambda: y_third(h))

    def stage(s, carry):
        pl.when(s == 1)(apply_step)
        v_pass(s)
        pl.when(s == 0)(first_stage)
        pl.when(s > 0)(lambda: later_stage(s))
        return carry

    lax.fori_loop(0, 3, stage, 0)

    top_all(0).wait_send()
    top_all(1).wait_send()
    for h in range(halves):
        x_sent(2, h)
        h_sent(2, h)
    y_sent(2, 0)
    y_sent(2, 1)


def solution(mesh):
    gx_n, gy_n, ha_n = mesh.shape["gx"], mesh.shape["gy"], mesh.shape["ha"]

    def body(level_set, wind_field):
        nx, ny, nh, nv = level_set.shape
        halves = ny // 8
        f32 = jnp.float32
        plain = pltpu.VMEM((nx, nh, ny, nv), f32)
        y_rows = -(-3 * nh // 8) * 8
        block_8 = pltpu.VMEM((nx, halves, nh, 8, nv), f32)
        dma = pltpu.SemaphoreType.DMA
        block = pltpu.with_memory_space_constraint(jnp.transpose(level_set, (0, 2, 1, 3)), pltpu.HBM)
        wind_field = pltpu.with_memory_space_constraint(wind_field, pltpu.HBM)
        out = pl.pallas_call(
            functools.partial(kernel, (gx_n, gy_n, ha_n, nx, nh, ny, nv)),
            out_shape=jax.ShapeDtypeStruct(block.shape, f32),
            in_specs=[
                pl.BlockSpec(memory_space=pltpu.HBM),
                pl.BlockSpec(memory_space=pltpu.HBM),
            ],
            out_specs=pl.BlockSpec(memory_space=pltpu.VMEM),
            scratch_shapes=[
                pltpu.VMEM((2, nx, ny), f32),
                pltpu.VMEM((3, nx, nh, ny + 16, nv), f32),
                plain,
                plain, plain, plain, plain, plain,
                pltpu.VMEM((3, halves, 3, nh, 8, nv), f32),
                pltpu.VMEM((3, halves, 3, nh, 8, nv), f32),
                pltpu.VMEM((3, halves, nx, 3, 8, nv), f32),
                pltpu.VMEM((3, halves, nx, 3, 8, nv), f32),
                pltpu.VMEM((3, nx, y_rows, nv), f32),
                pltpu.VMEM((3, nx, y_rows, nv), f32),
                pltpu.VMEM((3, 2, nx, y_rows, nv), f32),
                pltpu.VMEM((nh * ha_n, nv), f32),
                pltpu.VMEM((nh * ha_n, nv), f32),
                pltpu.VMEM((nx, ny, nv), f32),
                pltpu.VMEM((nx, ny, nv), f32),
                pltpu.VMEM((8, nv), f32),
                block_8, block_8, block_8, block_8, block_8, block_8, block_8, block_8,
                pltpu.VMEM((gx_n - 1, 8, nv), f32),
                pltpu.VMEM((gy_n - 1, 8, nv), f32),
                pltpu.VMEM((2, 8, nv), f32),
                dma((2,)),
                dma((halves, 2)), dma((2, halves, 2)),
                dma((halves, 2, 2)), dma((2, halves, 2, 2)),
                dma((2,)), dma((2, 2)),
                dma((2,)), dma((2,)),
            ],
            compiler_params=pltpu.CompilerParams(
                collective_id=0, has_side_effects=True, vmem_limit_bytes=VMEM_LIMIT),
        )(block, wind_field)
        return jnp.transpose(out * (2.0 / 3.0 / SCALE), (0, 2, 1, 3))

    return jax.shard_map(
        body,
        mesh=mesh,
        in_specs=(P("gx", "gy", "ha", None), P(None, "gx", "gy")),
        out_specs=P("gx", "gy", "ha", None),
        check_vma=False,
    )
```

```python
import functools
import math

import jax
import jax.numpy as jnp
import numpy as np
from jax import lax
from jax.experimental import pallas as pl
from jax.experimental.pallas import tpu as pltpu
from jax.sharding import PartitionSpec as P

CELL_SIZE = 0.05
SPEED_LOW = 0.1
SPEED_SPAN = 0.4
TURN_MAX = 1.0
ACCEL_MAX = 0.05
CFL_NUMBER = 0.5
WENO_EPS = 1e-06
SCALE = 64.0
VMEM_LIMIT = 40 * 2**20
V_ROWS = 2
V_APART = 12
MESH = pl.DeviceIdType.MESH


def eps_of(spacing):
    return 0.75 * WENO_EPS * (spacing * SCALE) ** 2


def one_side(b1, b2, b3, t1, t2):
    c1 = 3.0 * b1
    c3 = b3 + b3
    return b2 * (c3 * t1 + c1 * t2) / (b2 * (b3 + c1) + c1 * c3)


def both_sides(p, c, m, ta, tb):
    x = m * ta
    y = p * tb
    twice = 2.0 * (x + y)
    p2 = p + p
    m2 = m + m
    total = p + m
    far = 3.0 * (p2 * m)
    left = c * (twice + y) / (c * (total + p2) + far)
    right = c * (twice + x) / (c * (total + m2) + far)
    return left, right


def along(u, eps):
    n = len(u)
    q = [u[k + 1] - u[k] for k in range(n - 1)]
    d = [q[k + 1] - q[k] for k in range(n - 2)]
    s = [None] + [d[k] - d[k - 1] for k in range(1, n - 2)]
    t = [None] + [s[k + 1] - s[k] for k in range(1, n - 3)]
    z = [1.5 * (e * e) for e in d]
    p, c, m = [None], [None], [None]
    for k in range(1, n - 2):
        v = s[k] * s[k] + eps
        x = 0.75 * (d[k - 1] * d[k])
        w = v - x
        c.append(v + x)
        p.append(w + z[k])
        m.append(w + z[k - 1])
    return d, s, t, p, c, m


def kernel(
    sizes,
    u_hbm,
    wind_hbm,
    out_ref,
    wind,
    us,
    rate_0,
    acc,
    fx2,
    fx6,
    fy2,
    fy6,
    xlo,
    xhi,
    hlo,
    hhi,
    ylo,
    yhi,
    ysend,
    cos_t,
    sin_t,
    wx,
    wy,
    step_buf,
    vd,
    vq,
    vs,
    vc,
    vp,
    vm,
    vl,
    vr,
    top_x,
    top_y,
    top_send,
    in_sem,
    x_send,
    x_recv,
    h_send,
    h_recv,
    y_send,
    y_recv,
    top_send_sem,
    top_recv_sem,
):
    gx_n, gy_n, ha_n, nx, nh, ny, nv = sizes
    n_head = nh * ha_n
    d_theta = 2.0 * math.pi / n_head
    d_speed = SPEED_SPAN / nv
    gx, gy, ha = lax.axis_index("gx"), lax.axis_index("gy"), lax.axis_index("ha")
    below_x, above_x = gx > 0, gx < gx_n - 1
    below_y, above_y = gy > 0, gy < gy_n - 1
    h_up, h_down = lax.rem(ha + 1, ha_n), lax.rem(ha + ha_n - 1, ha_n)
    halves = ny // 8

    load_in = pltpu.make_async_copy(u_hbm, acc, in_sem.at[0])
    load_wind = pltpu.make_async_copy(wind_hbm, wind, in_sem.at[1])
    load_wind.start()
    load_in.start()

    barrier = pltpu.get_barrier_semaphore()
    for k in range(1, gx_n):
        pl.semaphore_signal(barrier, inc=1, device_id={"gx": lax.rem(gx + k, gx_n)}, device_id_type=MESH)
    for k in range(1, gy_n):
        pl.semaphore_signal(barrier, inc=1, device_id={"gy": lax.rem(gy + k, gy_n)}, device_id_type=MESH)
    pl.semaphore_signal(barrier, inc=1, device_id={"ha": h_up}, device_id_type=MESH)
    pl.semaphore_signal(barrier, inc=1, device_id={"ha": h_down}, device_id_type=MESH)

    def rows(h):
        return pl.ds(8 + 8 * h, 8)

    def inner(h):
        return pl.ds(8 * h, 8)

    def field(s):
        return (us.at[0], rate_0, us.at[2])[s]

    def parity(s):
        return s % 2 if isinstance(s, int) else lax.rem(s, 2)

    def base(s):
        return 0 if s == 1 else 8

    def x_copies(s, h, u=None, start=8):
        u = us.at[0] if u is None else u
        place = pl.ds(start + 8 * h, 8)
        down = pltpu.make_async_remote_copy(
            src_ref=u.at[pl.ds(0, 3), :, place, :], dst_ref=xhi.at[s, h],
            send_sem=x_send.at[h, 0], recv_sem=x_recv.at[parity(s), h, 0],
            device_id={"gx": gx - 1}, device_id_type=MESH)
        up = pltpu.make_async_remote_copy(
            src_ref=u.at[pl.ds(nx - 3, 3), :, place, :], dst_ref=xlo.at[s, h],
            send_sem=x_send.at[h, 1], recv_sem=x_recv.at[parity(s), h, 1],
            device_id={"gx": gx + 1}, device_id_type=MESH)
        return down, up

    def h_copies(s, h, g, u=None, start=8):
        u = us.at[0] if u is None else u
        place = pl.ds(start + 8 * h, 8)
        layers = pl.ds(g * (nx // 2), nx // 2)
        down = pltpu.make_async_remote_copy(
            src_ref=u.at[layers, pl.ds(0, 3), place, :], dst_ref=hhi.at[s, h, layers],
            send_sem=h_send.at[h, g, 0], recv_sem=h_recv.at[parity(s), h, g, 0],
            device_id={"ha": h_down}, device_id_type=MESH)
        up = pltpu.make_async_remote_copy(
            src_ref=u.at[layers, pl.ds(nh - 3, 3), place, :], dst_ref=hlo.at[s, h, layers],
            send_sem=h_send.at[h, g, 1], recv_sem=h_recv.at[parity(s), h, g, 1],
            device_id={"ha": h_up}, device_id_type=MESH)
        return down, up

    def y_copies(s):
        down = pltpu.make_async_remote_copy(
            src_ref=ysend.at[s, 0], dst_ref=yhi.at[s],
            send_sem=y_send.at[0], recv_sem=y_recv.at[parity(s), 0],
            device_id={"gy": gy - 1}, device_id_type=MESH)
        up = pltpu.make_async_remote_copy(
            src_ref=ysend.at[s, 1], dst_ref=ylo.at[s],
            send_sem=y_send.at[1], recv_sem=y_recv.at[parity(s), 1],
            device_id={"gy": gy + 1}, device_id_type=MESH)
        return down, up

    def x_sent(s, h):
        down, up = x_copies(s, h, field(s), base(s))
        pl.when(below_x)(down.wait_send)
        pl.when(above_x)(up.wait_send)

    def h_sent(s, h):
        for g in range(2):
            for copy in h_copies(s, h, g, field(s), base(s)):
                copy.wait_send()

    def y_sent(s, which):
        pl.when((below_y, above_y)[which])(y_copies(s)[which].wait_send)

    def start_half(s, h):
        if s > 0:
            x_sent(s - 1, h)
            h_sent(s - 1, h)
        for g in range(2):
            for copy in h_copies(s, h, g, field(s), base(s)):
                copy.start()
        down, up = x_copies(s, h, field(s), base(s))
        pl.when(below_x)(down.start)
        pl.when(above_x)(up.start)

    def start_y(s, which):
        if s > 0:
            y_sent(s - 1, which)
        pl.when((below_y, above_y)[which])(y_copies(s)[which].start)

    angles = lax.broadcasted_iota(jnp.int32, (n_head, nv), 0).astype(jnp.float32) * d_theta
    cos_t[...] = jnp.cos(angles)
    sin_t[...] = jnp.sin(angles)

    low = np.float32(SPEED_LOW) + np.float32(SPEED_SPAN) * np.float32(0.5) / np.float32(nv)
    high = np.float32(SPEED_LOW) + np.float32(SPEED_SPAN) * np.float32(nv - 0.5) / np.float32(nv)
    load_wind.wait()
    wind_x, wind_y = wind[0], wind[1]

    def rate_of(k, top):
        c = jnp.broadcast_to(cos_t[pl.ds(k, 1), 0:ny], (nx, ny))
        n = jnp.broadcast_to(sin_t[pl.ds(k, 1), 0:ny], (nx, ny))
        for speed in (float(low), float(high)):
            top = jnp.maximum(top, jnp.abs(speed * c + wind_x) + jnp.abs(speed * n + wind_y))
        return top

    top = lax.fori_loop(0, n_head, rate_of, jnp.zeros((nx, ny), jnp.float32), unroll=4)
    top_send[0] = jnp.full((8, nv), jnp.max(top), jnp.float32)


    def top_copy(axis, me, size, k, phase):
        buf = (top_x, top_y)[phase]
        return pltpu.make_async_remote_copy(
            src_ref=top_send.at[phase], dst_ref=buf.at[k - 1],
            send_sem=top_send_sem.at[phase], recv_sem=top_recv_sem.at[phase],
            device_id={axis: lax.rem(me + k, size)}, device_id_type=MESH)

    def top_all(phase):
        buf = (top_x, top_y)[phase]
        axis, me, size = (("gx", gx, gx_n), ("gy", gy, gy_n))[phase]
        return pltpu.make_async_remote_copy(
            src_ref=buf, dst_ref=buf, send_sem=top_send_sem.at[phase], recv_sem=top_recv_sem.at[phase],
            device_id={axis: lax.rem(me + 1, size)}, device_id_type=MESH)

    top_copies = [
        [top_copy("gx", gx, gx_n, k, 0) for k in range(1, gx_n)],
        [top_copy("gy", gy, gy_n, k, 1) for k in range(1, gy_n)],
    ]
    load_in.wait()

    def pack_y(s, i):
        u = us.at[s]
        for j in range(nh):
            ysend[s, 0, i, pl.ds(3 * j, 3), :] = u[i, j, pl.ds(8, 3), :]
            ysend[s, 1, i, pl.ds(3 * j, 3), :] = u[i, j, pl.ds(8 + ny - 3, 3), :]

    def scale_in(i, carry):
        for j in range(nh):
            us[0, i, j, pl.ds(8, ny), :] = acc[i, j] * SCALE
        return carry

    lax.fori_loop(0, nx, scale_in, 0)

    def pack_all(s):
        def body(i, carry):
            pack_y(s, i)
            return carry
        lax.fori_loop(0, nx, body, 0)

    pack_all(0)

    pl.semaphore_wait(barrier, gx_n - 1 + gy_n - 1 + 2)
    for copy in top_copies[0]:
        copy.start()
    start_half(0, 0)
    start_y(0, 0)
    start_y(0, 1)


    diagonal = lax.broadcasted_iota(jnp.int32, (ny, ny), 0) == lax.broadcasted_iota(jnp.int32, (ny, ny), 1)
    for i in range(nx):
        for part, out in ((0, wx), (1, wy)):
            row = jnp.broadcast_to(wind[part, pl.ds(i, 1), :], (ny, ny))
            column = jnp.sum(jnp.where(diagonal, row, 0.0), axis=1, keepdims=True)
            out[i] = jnp.broadcast_to(column, (ny, nv))

    speeds = SPEED_LOW + SPEED_SPAN * (
        lax.broadcasted_iota(jnp.int32, (1, nv), 1).astype(jnp.float32) + 0.5) / nv

    def flow_of(j, carry):
        c = speeds * cos_t[pl.ds(ha * nh + j, 1), :]
        n = speeds * sin_t[pl.ds(ha * nh + j, 1), :]
        for i in range(nx):
            f = c + wx[i]
            fx2[i, j] = f * (0.5 / CELL_SIZE)
            fx6[i, j] = jnp.abs(f) * (1.0 / (6.0 * CELL_SIZE))
            f = n + wy[i]
            fy2[i, j] = f * (0.5 / CELL_SIZE)
            fy6[i, j] = jnp.abs(f) * (1.0 / (6.0 * CELL_SIZE))
        return carry

    lax.fori_loop(0, nh, flow_of, 0)
    step_buf[...] = jnp.ones_like(step_buf)

    def v_pass(s):
        u = us.at[s]
        eps = eps_of(d_speed)
        e2 = eps * eps
        factor = ACCEL_MAX / (6.0 * d_speed)
        blocks = [(i, h, g) for i in range(nx) for h in range(halves) for g in range(nh // V_ROWS)]
        shape = (V_ROWS, 8, nv)
        lane = lax.broadcasted_iota(jnp.int32, (8, nv), 1)
        first = jnp.broadcast_to(lane == 0, shape)
        last = jnp.broadcast_to(lane == nv - 1, shape)

        def level_0(i, h, g):
            part = pl.ds(V_ROWS * g, V_ROWS)
            v = u[i, part, rows(h), :]
            a = pltpu.roll(v, nv - 1, 2) - v
            b = v - pltpu.roll(v, 1, 2)
            q1 = jnp.where(last, b, a)
            q0 = jnp.where(first, a, b)
            vq[i, h, part] = 3.0 * (q0 + q1)
            vd[i, h, part] = q1 - q0

        def level_1(i, h, g):
            part = pl.ds(V_ROWS * g, V_ROWS)
            d = vd[i, h, part]
            dm = pltpu.roll(d, 1, 2)
            s = d - dm
            c = (s * s + eps) + 0.75 * (d * dm)
            r = 1.5 * s
            p = c + r * d
            m = c - r * dm
            vs[i, h, part] = s
            vc[i, h, part] = c * c
            vp[i, h, part] = p * p
            vm[i, h, part] = m * m

        def level_2(i, h, g):
            part = pl.ds(V_ROWS * g, V_ROWS)
            s = vs[i, h, part]
            ta = s - pltpu.roll(s, 1, 2)
            tb = pltpu.roll(s, nv - 1, 2) - s
            p = pltpu.roll(vp[i, h, part], 1, 2)
            m = pltpu.roll(vm[i, h, part], nv - 1, 2)
            c = vc[i, h, part]
            left = one_side(jnp.where(first, e2, p), c, m, jnp.where(first, 0.0, ta), tb)
            right = one_side(jnp.where(first, e2, m), c, p, jnp.where(first, 0.0, tb), ta)
            vl[i, h, part] = left + s
            vr[i, h, part] = right - s

        def level_3(i, h, g):
            part = pl.ds(V_ROWS * g, V_ROWS)
            right = pltpu.roll(vr[i, h, part], nv - 1, 2)
            d3 = vq[i, h, part]
            acc[i, part, inner(h), :] = factor * jnp.maximum(d3 + right, vl[i, h, part] - d3)

        levels = (level_0, level_1, level_2, level_3)
        apart = V_APART
        for step in range(len(blocks) + apart * (len(levels) - 1)):
            for n in reversed(range(len(levels))):
                k = step - apart * n
                if 0 <= k < len(blocks):
                    levels[n](*blocks[k])

    def h_pass(s, h, g):
        u = us.at[s]
        factor = TURN_MAX / (6.0 * d_theta)

        def body(i, carry):
            cells = [hlo[s, h, i, k] for k in range(3)]
            cells += [u[i, k, rows(h), :] for k in range(nh)]
            cells += [hhi[s, h, i, k] for k in range(3)]
            d, sd, t, p, c, m = along(cells, eps_of(d_theta))
            square = lambda r: [None] + [e * e for e in r[1:]]
            p, c, m = square(p), square(c), square(m)
            sides = {}
            for k in range(2, nh + 3):
                sides[k] = both_sides(p[k - 1], c[k], m[k + 1], t[k - 1], t[k])
            for j in range(nh):
                k = j + 2
                d3 = 3.0 * (cells[j + 4] - cells[j + 2])
                value = jnp.maximum(d3 + (sides[k + 1][1] - sd[k + 1]), (sides[k][0] + sd[k]) - d3)
                acc[i, j, inner(h), :] += factor * value
            return carry

        lax.fori_loop(g * (nx // 2), (g + 1) * (nx // 2), body, 0, unroll=2)

    def x_pass(s, h, store):
        u = us.at[s]

        def body(j, carry):
            cells = [xlo[s, h, k, j] for k in range(3)]
            cells += [u[k, j, rows(h), :] for k in range(nx)]
            cells += [xhi[s, h, k, j] for k in range(3)]
            d, sd, t, p, c, m = along(cells, eps_of(CELL_SIZE))
            for i in range(nx):
                k = i + 2
                f2 = fx2[i, j, inner(h), :]
                ahead = f2 > 0.0
                b1 = jnp.where(ahead, m[k + 2], p[k - 1])
                b2 = jnp.where(ahead, c[k + 1], c[k])
                b3 = jnp.where(ahead, p[k], m[k + 1])
                t1 = jnp.where(ahead, t[k + 1], t[k - 1])
                dd = d[k] - jnp.where(ahead, d[k + 1], d[k - 1])
                fix = one_side(b1 * b1, b2 * b2, b3 * b3, t1, t[k])
                term = f2 * (cells[i + 4] - cells[i + 2]) + fx6[i, j, inner(h), :] * (dd + fix)
                store(i, j, h, acc[i, j, inner(h), :] + term)
            return carry

        lax.fori_loop(0, nh, body, 0, unroll=2)

    def y_value(cells, f2, f6):
        eps = eps_of(CELL_SIZE)
        ahead = f2 > 0.0
        q = [cells[k + 1] - cells[k] for k in range(6)]
        d = [q[k + 1] - q[k] for k in range(5)]
        e1 = jnp.where(ahead, d[4], d[0])
        e2 = jnp.where(ahead, d[3], d[1])
        e3 = d[2]
        e4 = jnp.where(ahead, d[1], d[3])
        s1, s2, s3 = e2 - e1, e3 - e2, e4 - e3
        e2k, e3k = 0.75 * e2, 0.75 * e3
        b1 = (s1 * s1 + eps) + e2k * (e2 + s1)
        b2 = (s2 * s2 + eps) + e2k * e3
        b3 = (s3 * s3 + eps) + e3k * (e3 - s3)
        fix = one_side(b1 * b1, b2 * b2, b3 * b3, s2 - s1, s3 - s2)
        return f2 * (cells[4] - cells[2]) + f6 * (s2 + fix)

    def y_term(u, i, j, h):
        cells = [u[i, j, pl.ds(8 + 8 * h + r, 8), :] for r in range(-3, 4)]
        return y_value(cells, fy2[i, j, inner(h), :], fy6[i, j, inner(h), :])

    def add_up(i, j, h, total):
        acc[i, j, inner(h), :] = total

    def keep_rate(i, j, h, total):
        rate_0[i, j, inner(h), :] = jnp.minimum(total, 0.0)

    def y_inner():
        u = us.at[0]

        def body(i, carry):
            for j in range(nh):
                cells = [u[i, j, pl.ds(11 + r, 8), :] for r in range(-3, 4)]
                acc[i, j, pl.ds(3, 8), :] += y_value(cells, fy2[i, j, pl.ds(3, 8), :], fy6[i, j, pl.ds(3, 8), :])
            return carry

        lax.fori_loop(0, nx, body, 0, unroll=2)

    def y_outer():
        u = us.at[0]
        low = lax.broadcasted_iota(jnp.int32, (8, nv), 0) < 3

        def body(i, carry):
            for j in range(nh):
                cells = [jnp.where(low, u[i, j, pl.ds(8 + r, 8), :], u[i, j, pl.ds(16 + r, 8), :]) for r in range(-3, 4)]
                f2 = jnp.where(low, fy2[i, j, inner(0), :], fy2[i, j, inner(1), :])
                f6 = jnp.where(low, fy6[i, j, inner(0), :], fy6[i, j, inner(1), :])
                value = y_value(cells, f2, f6)
                acc[i, j, inner(0), :] += jnp.where(low, value, 0.0)
                acc[i, j, inner(1), :] += jnp.where(low, 0.0, value)
            return carry

        lax.fori_loop(0, nx, body, 0, unroll=2)

    def pack_first(h):
        def body(i, carry):
            for j in range(nh):
                if h == 0:
                    ysend[1, 0, i, pl.ds(3 * j, 3), :] = rate_0[i, j, 0:3, :]
                if h == halves - 1:
                    ysend[1, 1, i, pl.ds(3 * j, 3), :] = rate_0[i, j, ny - 3:ny, :]
            return carry

        lax.fori_loop(0, nx, body, 0)

    def y_second(h):
        dt = 0.25 * step_buf[...]

        def body(i, carry):
            for j in range(nh):
                change = jnp.minimum(acc[i, j, inner(h), :] + y_term(us.at[1], i, j, h), 0.0)
                fresh = (0.75 * us[0, i, j, rows(h), :] + 0.25 * us[1, i, j, rows(h), :]) + dt * change
                us[2, i, j, rows(h), :] = fresh
                if h == 0:
                    ysend[2, 0, i, pl.ds(3 * j, 3), :] = fresh[0:3]
                if h == halves - 1:
                    ysend[2, 1, i, pl.ds(3 * j, 3), :] = fresh[5:8]
            return carry

        x_sent(1, h)
        h_sent(1, h)
        down, up = x_copies(2, h, field(2), base(2))
        for g in range(2):
            lax.fori_loop(g * (nx // 2), (g + 1) * (nx // 2), body, 0, unroll=2)
            for copy in h_copies(2, h, g, field(2), base(2)):
                copy.start()
            if g == 0:
                pl.when(below_x)(down.start)
            else:
                pl.when(above_x)(up.start)
        if h == 0:
            start_y(2, 0)
        if h == halves - 1:
            start_y(2, 1)

    def y_third(h):
        dt = step_buf[...]

        def body(i, carry):
            for j in range(nh):
                change = jnp.minimum(acc[i, j, inner(h), :] + y_term(us.at[2], i, j, h), 0.0)
                out_ref[i, j, inner(h), :] = (us[2, i, j, rows(h), :] - us[0, i, j, rows(h), :]) + dt * change
            return carry

        lax.fori_loop(0, nx, body, 0, unroll=2)

    def receive_x(s, h):
        u = us.at[s]
        down, up = x_copies(s, h)
        pl.when(above_x)(down.wait_recv)
        pl.when(below_x)(up.wait_recv)

        def stepped(halo):
            def body(k, carry):
                dt = step_buf[...]
                for j in range(nh):
                    halo[1, h, k, j] = halo[0, h, k, j] + dt * halo[1, h, k, j]
                return carry
            lax.fori_loop(0, 3, body, 0)

        pl.when(jnp.logical_and(s == 1, above_x))(lambda: stepped(xhi))
        pl.when(jnp.logical_and(s == 1, below_x))(lambda: stepped(xlo))

        @pl.when(jnp.logical_not(below_x))
        def _():
            def body(j, carry):
                edge = u[0, j, rows(h), :]
                slope = edge - u[1, j, rows(h), :]
                for r in (1, 2, 3):
                    xlo[s, h, 3 - r, j] = edge + float(r) * slope
                return carry
            lax.fori_loop(0, nh, body, 0)

        @pl.when(jnp.logical_not(above_x))
        def _():
            def body(j, carry):
                edge = u[nx - 1, j, rows(h), :]
                slope = edge - u[nx - 2, j, rows(h), :]
                for r in (1, 2, 3):
                    xhi[s, h, r - 1, j] = edge + float(r) * slope
                return carry
            lax.fori_loop(0, nh, body, 0)

    def receive_h(s, h, g):
        for copy in h_copies(s, h, g):
            copy.wait_recv()

        @pl.when(s == 1)
        def _():
            def body(i, carry):
                dt = step_buf[...]
                for k in range(3):
                    hlo[1, h, i, k] = hlo[0, h, i, k] + dt * hlo[1, h, i, k]
                    hhi[1, h, i, k] = hhi[0, h, i, k] + dt * hhi[1, h, i, k]
                return carry
            lax.fori_loop(g * (nx // 2), (g + 1) * (nx // 2), body, 0)

    def receive_y(s, which):
        u = us.at[s]
        copy = y_copies(s)[which]
        there = (above_y, below_y)[which]

        @pl.when(there)
        def _():
            copy.wait_recv()

            halo = (yhi, ylo)[which]
            place = pl.ds((8 + ny, 5)[which], 3)

            @pl.when(s == 1)
            def _():
                def body(i, carry):
                    halo[1, i] = halo[0, i] + step_buf[0:1, :] * halo[1, i]
                    return carry
                lax.fori_loop(0, nx, body, 0)

            def body(i, carry):
                for j in range(nh):
                    u[i, j, place, :] = halo[s, i, pl.ds(3 * j, 3), :]
                return carry
            lax.fori_loop(0, nx, body, 0)

        @pl.when(jnp.logical_not(there))
        def _():
            def body(i, carry):
                for j in range(nh):
                    if which == 0:
                        edge = u[i, j, pl.ds(8 + ny - 1, 1), :]
                        slope = edge - u[i, j, pl.ds(8 + ny - 2, 1), :]
                        for r in (1, 2, 3):
                            u[i, j, pl.ds(8 + ny - 1 + r, 1), :] = edge + float(r) * slope
                    else:
                        edge = u[i, j, pl.ds(8, 1), :]
                        slope = edge - u[i, j, pl.ds(9, 1), :]
                        for r in (1, 2, 3):
                            u[i, j, pl.ds(8 - r, 1), :] = edge + float(r) * slope
                return carry
            lax.fori_loop(0, nx, body, 0)

    def apply_step():
        top_all(1).wait_recv()
        best = top_send[1]
        for k in range(1, gy_n):
            best = jnp.maximum(best, top_y[k - 1])
        rate = best / CELL_SIZE + (TURN_MAX / d_theta + ACCEL_MAX / d_speed)
        dt = CFL_NUMBER / rate
        step_buf[...] = dt

        def body(i, carry):
            fresh = [us[0, i, j, rows(h), :] + dt * rate_0[i, j, inner(h), :] for j in range(nh) for h in range(halves)]
            for j in range(nh):
                for h in range(halves):
                    us[1, i, j, rows(h), :] = fresh[j * halves + h]
            return carry

        lax.fori_loop(0, nx, body, 0)

    def second_rates():
        top_all(0).wait_recv()
        best = top_send[0]
        for k in range(1, gx_n):
            best = jnp.maximum(best, top_x[k - 1])
        top_send[1] = best
        for copy in top_copies[1]:
            copy.start()

    def first_stage():
        for h in range(1, halves):
            start_half(0, h)
        y_inner()
        second_rates()
        receive_y(0, 0)
        receive_y(0, 1)
        y_outer()
        for h in range(halves):
            for g in range(2):
                receive_h(0, h, g)
                h_pass(0, h, g)
            receive_x(0, h)
            x_pass(0, h, keep_rate)
            pack_first(h)
            start_half(1, h)
            if h == 0:
                start_y(1, 0)
            if h == halves - 1:
                start_y(1, 1)

    def later_stage(s):
        for h in range(halves):
            for g in range(2):
                receive_h(s, h, g)
                h_pass(s, h, g)
            receive_x(s, h)
            x_pass(s, h, add_up)
            if h == 0:
                receive_y(s, 1)
            if h == halves - 1:
                receive_y(s, 0)
            pl.when(s == 1)(lambda: y_second(h))
            pl.when(s == 2)(lambda: y_third(h))

    def stage(s, carry):
        pl.when(s == 1)(apply_step)
        v_pass(s)
        pl.when(s == 0)(first_stage)
        pl.when(s > 0)(lambda: later_stage(s))
        return carry

    lax.fori_loop(0, 3, stage, 0)

    top_all(0).wait_send()
    top_all(1).wait_send()
    for h in range(halves):
        x_sent(2, h)
        h_sent(2, h)
    y_sent(2, 0)
    y_sent(2, 1)


def solution(mesh):
    gx_n, gy_n, ha_n = mesh.shape["gx"], mesh.shape["gy"], mesh.shape["ha"]

    def body(level_set, wind_field):
        nx, ny, nh, nv = level_set.shape
        halves = ny // 8
        f32 = jnp.float32
        plain = pltpu.VMEM((nx, nh, ny, nv), f32)
        y_rows = -(-3 * nh // 8) * 8
        block_8 = pltpu.VMEM((nx, halves, nh, 8, nv), f32)
        dma = pltpu.SemaphoreType.DMA
        block = pltpu.with_memory_space_constraint(jnp.transpose(level_set, (0, 2, 1, 3)), pltpu.HBM)
        wind_field = pltpu.with_memory_space_constraint(wind_field, pltpu.HBM)
        out = pl.pallas_call(
            functools.partial(kernel, (gx_n, gy_n, ha_n, nx, nh, ny, nv)),
            out_shape=jax.ShapeDtypeStruct(block.shape, f32),
            in_specs=[
                pl.BlockSpec(memory_space=pltpu.HBM),
                pl.BlockSpec(memory_space=pltpu.HBM),
            ],
            out_specs=pl.BlockSpec(memory_space=pltpu.VMEM),
            scratch_shapes=[
                pltpu.VMEM((2, nx, ny), f32),
                pltpu.VMEM((3, nx, nh, ny + 16, nv), f32),
                plain,
                plain, plain, plain, plain, plain,
                pltpu.VMEM((3, halves, 3, nh, 8, nv), f32),
                pltpu.VMEM((3, halves, 3, nh, 8, nv), f32),
                pltpu.VMEM((3, halves, nx, 3, 8, nv), f32),
                pltpu.VMEM((3, halves, nx, 3, 8, nv), f32),
                pltpu.VMEM((3, nx, y_rows, nv), f32),
                pltpu.VMEM((3, nx, y_rows, nv), f32),
                pltpu.VMEM((3, 2, nx, y_rows, nv), f32),
                pltpu.VMEM((nh * ha_n, nv), f32),
                pltpu.VMEM((nh * ha_n, nv), f32),
                pltpu.VMEM((nx, ny, nv), f32),
                pltpu.VMEM((nx, ny, nv), f32),
                pltpu.VMEM((8, nv), f32),
                block_8, block_8, block_8, block_8, block_8, block_8, block_8, block_8,
                pltpu.VMEM((gx_n - 1, 8, nv), f32),
                pltpu.VMEM((gy_n - 1, 8, nv), f32),
                pltpu.VMEM((2, 8, nv), f32),
                dma((2,)),
                dma((halves, 2)), dma((2, halves, 2)),
                dma((halves, 2, 2)), dma((2, halves, 2, 2)),
                dma((2,)), dma((2, 2)),
                dma((2,)), dma((2,)),
            ],
            compiler_params=pltpu.CompilerParams(
                collective_id=0, has_side_effects=True, vmem_limit_bytes=VMEM_LIMIT),
        )(block, wind_field)
        return jnp.transpose(out * (2.0 / 3.0 / SCALE), (0, 2, 1, 3))

    return jax.shard_map(
        body,
        mesh=mesh,
        in_specs=(P("gx", "gy", "ha", None), P(None, "gx", "gy")),
        out_specs=P("gx", "gy", "ha", None),
        check_vma=False,
    )
```

```python
import functools
import math

import jax
import jax.numpy as jnp
import numpy as np
from jax import lax
from jax.experimental import pallas as pl
from jax.experimental.pallas import tpu as pltpu
from jax.sharding import PartitionSpec as P

CELL_SIZE = 0.05
SPEED_LOW = 0.1
SPEED_SPAN = 0.4
TURN_MAX = 1.0
ACCEL_MAX = 0.05
CFL_NUMBER = 0.5
WENO_EPS = 1e-06
SCALE = 64.0
VMEM_LIMIT = 40 * 2**20
V_ROWS = 2
V_APART = 12
MESH = pl.DeviceIdType.MESH


def eps_of(spacing):
    return 0.75 * WENO_EPS * (spacing * SCALE) ** 2


def one_side(b1, b2, b3, t1, t2):
    c1 = 3.0 * b1
    c3 = b3 + b3
    return b2 * (c3 * t1 + c1 * t2) / (b2 * (b3 + c1) + c1 * c3)


def both_sides(p, c, m, ta, tb):
    x = m * ta
    y = p * tb
    twice = 2.0 * (x + y)
    p2 = p + p
    m2 = m + m
    total = p + m
    far = 3.0 * (p2 * m)
    left = c * (twice + y) / (c * (total + p2) + far)
    right = c * (twice + x) / (c * (total + m2) + far)
    return left, right


def along(u, eps):
    n = len(u)
    q = [u[k + 1] - u[k] for k in range(n - 1)]
    d = [q[k + 1] - q[k] for k in range(n - 2)]
    s = [None] + [d[k] - d[k - 1] for k in range(1, n - 2)]
    t = [None] + [s[k + 1] - s[k] for k in range(1, n - 3)]
    z = [1.5 * (e * e) for e in d]
    p, c, m = [None], [None], [None]
    for k in range(1, n - 2):
        v = s[k] * s[k] + eps
        x = 0.75 * (d[k - 1] * d[k])
        w = v - x
        c.append(v + x)
        p.append(w + z[k])
        m.append(w + z[k - 1])
    return d, s, t, p, c, m


def kernel(
    sizes,
    u_hbm,
    wind_hbm,
    out_ref,
    wind,
    us,
    rate_0,
    acc,
    fx2,
    fx6,
    fy2,
    fy6,
    xlo,
    xhi,
    hlo,
    hhi,
    ylo,
    yhi,
    ysend,
    cos_t,
    sin_t,
    wx,
    wy,
    step_buf,
    vd,
    vq,
    vs,
    vc,
    vp,
    vm,
    vl,
    vr,
    top_x,
    top_y,
    top_send,
    in_sem,
    x_send,
    x_recv,
    h_send,
    h_recv,
    y_send,
    y_recv,
    top_send_sem,
    top_recv_sem,
):
    gx_n, gy_n, ha_n, nx, nh, ny, nv = sizes
    n_head = nh * ha_n
    d_theta = 2.0 * math.pi / n_head
    d_speed = SPEED_SPAN / nv
    gx, gy, ha = lax.axis_index("gx"), lax.axis_index("gy"), lax.axis_index("ha")
    below_x, above_x = gx > 0, gx < gx_n - 1
    below_y, above_y = gy > 0, gy < gy_n - 1
    h_up, h_down = lax.rem(ha + 1, ha_n), lax.rem(ha + ha_n - 1, ha_n)
    halves = ny // 8

    load_in = pltpu.make_async_copy(u_hbm, acc, in_sem.at[0])
    load_wind = pltpu.make_async_copy(wind_hbm, wind, in_sem.at[1])
    load_wind.start()
    load_in.start()

    barrier = pltpu.get_barrier_semaphore()
    for k in range(1, gx_n):
        pl.semaphore_signal(barrier, inc=1, device_id={"gx": lax.rem(gx + k, gx_n)}, device_id_type=MESH)
    for k in range(1, gy_n):
        pl.semaphore_signal(barrier, inc=1, device_id={"gy": lax.rem(gy + k, gy_n)}, device_id_type=MESH)
    pl.semaphore_signal(barrier, inc=1, device_id={"ha": h_up}, device_id_type=MESH)
    pl.semaphore_signal(barrier, inc=1, device_id={"ha": h_down}, device_id_type=MESH)

    def rows(h):
        return pl.ds(8 + 8 * h, 8)

    def inner(h):
        return pl.ds(8 * h, 8)

    def field(s):
        return (us.at[0], rate_0, us.at[2])[s]

    def parity(s):
        return s % 2 if isinstance(s, int) else lax.rem(s, 2)

    def base(s):
        return 0 if s == 1 else 8

    def x_copies(s, h, u=None, start=8):
        u = us.at[0] if u is None else u
        place = pl.ds(start + 8 * h, 8)
        down = pltpu.make_async_remote_copy(
            src_ref=u.at[pl.ds(0, 3), :, place, :], dst_ref=xhi.at[s, h],
            send_sem=x_send.at[h, 0], recv_sem=x_recv.at[parity(s), h, 0],
            device_id={"gx": gx - 1}, device_id_type=MESH)
        up = pltpu.make_async_remote_copy(
            src_ref=u.at[pl.ds(nx - 3, 3), :, place, :], dst_ref=xlo.at[s, h],
            send_sem=x_send.at[h, 1], recv_sem=x_recv.at[parity(s), h, 1],
            device_id={"gx": gx + 1}, device_id_type=MESH)
        return down, up

    def h_copies(s, h, g, u=None, start=8):
        u = us.at[0] if u is None else u
        place = pl.ds(start + 8 * h, 8)
        layers = pl.ds(g * (nx // 2), nx // 2)
        down = pltpu.make_async_remote_copy(
            src_ref=u.at[layers, pl.ds(0, 3), place, :], dst_ref=hhi.at[s, h, layers],
            send_sem=h_send.at[h, g, 0], recv_sem=h_recv.at[parity(s), h, g, 0],
            device_id={"ha": h_down}, device_id_type=MESH)
        up = pltpu.make_async_remote_copy(
            src_ref=u.at[layers, pl.ds(nh - 3, 3), place, :], dst_ref=hlo.at[s, h, layers],
            send_sem=h_send.at[h, g, 1], recv_sem=h_recv.at[parity(s), h, g, 1],
            device_id={"ha": h_up}, device_id_type=MESH)
        return down, up

    def y_copies(s):
        down = pltpu.make_async_remote_copy(
            src_ref=ysend.at[s, 0], dst_ref=yhi.at[s],
            send_sem=y_send.at[0], recv_sem=y_recv.at[parity(s), 0],
            device_id={"gy": gy - 1}, device_id_type=MESH)
        up = pltpu.make_async_remote_copy(
            src_ref=ysend.at[s, 1], dst_ref=ylo.at[s],
            send_sem=y_send.at[1], recv_sem=y_recv.at[parity(s), 1],
            device_id={"gy": gy + 1}, device_id_type=MESH)
        return down, up

    def x_sent(s, h):
        down, up = x_copies(s, h, field(s), base(s))
        pl.when(below_x)(down.wait_send)
        pl.when(above_x)(up.wait_send)

    def h_sent(s, h):
        for g in range(2):
            for copy in h_copies(s, h, g, field(s), base(s)):
                copy.wait_send()

    def y_sent(s, which):
        pl.when((below_y, above_y)[which])(y_copies(s)[which].wait_send)

    def start_half(s, h):
        if s > 0:
            x_sent(s - 1, h)
            h_sent(s - 1, h)
        for g in range(2):
            for copy in h_copies(s, h, g, field(s), base(s)):
                copy.start()
        down, up = x_copies(s, h, field(s), base(s))
        pl.when(below_x)(down.start)
        pl.when(above_x)(up.start)

    def start_y(s, which):
        if s > 0:
            y_sent(s - 1, which)
        pl.when((below_y, above_y)[which])(y_copies(s)[which].start)

    angles = lax.broadcasted_iota(jnp.int32, (n_head, nv), 0).astype(jnp.float32) * d_theta
    cos_t[...] = jnp.cos(angles)
    sin_t[...] = jnp.sin(angles)

    low = np.float32(SPEED_LOW) + np.float32(SPEED_SPAN) * np.float32(0.5) / np.float32(nv)
    high = np.float32(SPEED_LOW) + np.float32(SPEED_SPAN) * np.float32(nv - 0.5) / np.float32(nv)
    load_wind.wait()
    wind_x, wind_y = wind[0], wind[1]

    def rate_of(k, top):
        c = jnp.broadcast_to(cos_t[pl.ds(k, 1), 0:ny], (nx, ny))
        n = jnp.broadcast_to(sin_t[pl.ds(k, 1), 0:ny], (nx, ny))
        for speed in (float(low), float(high)):
            top = jnp.maximum(top, jnp.abs(speed * c + wind_x) + jnp.abs(speed * n + wind_y))
        return top

    top = lax.fori_loop(0, n_head, rate_of, jnp.zeros((nx, ny), jnp.float32), unroll=4)
    top_send[0] = jnp.full((8, nv), jnp.max(top), jnp.float32)


    def top_copy(axis, me, size, k, phase):
        buf = (top_x, top_y)[phase]
        return pltpu.make_async_remote_copy(
            src_ref=top_send.at[phase], dst_ref=buf.at[k - 1],
            send_sem=top_send_sem.at[phase], recv_sem=top_recv_sem.at[phase],
            device_id={axis: lax.rem(me + k, size)}, device_id_type=MESH)

    def top_all(phase):
        buf = (top_x, top_y)[phase]
        axis, me, size = (("gx", gx, gx_n), ("gy", gy, gy_n))[phase]
        return pltpu.make_async_remote_copy(
            src_ref=buf, dst_ref=buf, send_sem=top_send_sem.at[phase], recv_sem=top_recv_sem.at[phase],
            device_id={axis: lax.rem(me + 1, size)}, device_id_type=MESH)

    top_copies = [
        [top_copy("gx", gx, gx_n, k, 0) for k in range(1, gx_n)],
        [top_copy("gy", gy, gy_n, k, 1) for k in range(1, gy_n)],
    ]
    load_in.wait()

    def pack_y(s, i):
        u = us.at[s]
        for j in range(nh):
            ysend[s, 0, i, pl.ds(3 * j, 3), :] = u[i, j, pl.ds(8, 3), :]
            ysend[s, 1, i, pl.ds(3 * j, 3), :] = u[i, j, pl.ds(8 + ny - 3, 3), :]

    def scale_in(i, carry):
        for j in range(nh):
            us[0, i, j, pl.ds(8, ny), :] = acc[i, j] * SCALE
        return carry

    lax.fori_loop(0, nx, scale_in, 0)

    def pack_all(s):
        def body(i, carry):
            pack_y(s, i)
            return carry
        lax.fori_loop(0, nx, body, 0)

    pack_all(0)

    pl.semaphore_wait(barrier, gx_n - 1 + gy_n - 1 + 2)
    for copy in top_copies[0]:
        copy.start()
    start_half(0, 0)
    start_y(0, 0)
    start_y(0, 1)


    diagonal = lax.broadcasted_iota(jnp.int32, (ny, ny), 0) == lax.broadcasted_iota(jnp.int32, (ny, ny), 1)
    for i in range(nx):
        for part, out in ((0, wx), (1, wy)):
            row = jnp.broadcast_to(wind[part, pl.ds(i, 1), :], (ny, ny))
            column = jnp.sum(jnp.where(diagonal, row, 0.0), axis=1, keepdims=True)
            out[i] = jnp.broadcast_to(column, (ny, nv))

    speeds = SPEED_LOW + SPEED_SPAN * (
        lax.broadcasted_iota(jnp.int32, (1, nv), 1).astype(jnp.float32) + 0.5) / nv

    def flow_of(j, carry):
        c = speeds * cos_t[pl.ds(ha * nh + j, 1), :]
        n = speeds * sin_t[pl.ds(ha * nh + j, 1), :]
        for i in range(nx):
            f = c + wx[i]
            fx2[i, j] = f * (0.5 / CELL_SIZE)
            fx6[i, j] = jnp.abs(f) * (1.0 / (6.0 * CELL_SIZE))
            f = n + wy[i]
            fy2[i, j] = f * (0.5 / CELL_SIZE)
            fy6[i, j] = jnp.abs(f) * (1.0 / (6.0 * CELL_SIZE))
        return carry

    lax.fori_loop(0, nh, flow_of, 0)
    step_buf[...] = jnp.ones_like(step_buf)

    def v_pass(s):
        u = us.at[s]
        eps = eps_of(d_speed)
        e2 = eps * eps
        factor = ACCEL_MAX / (6.0 * d_speed)
        blocks = [(i, h, g) for i in range(nx) for h in range(halves) for g in range(nh // V_ROWS)]
        shape = (V_ROWS, 8, nv)
        lane = lax.broadcasted_iota(jnp.int32, (8, nv), 1)
        first = jnp.broadcast_to(lane == 0, shape)
        last = jnp.broadcast_to(lane == nv - 1, shape)

        def level_0(i, h, g):
            part = pl.ds(V_ROWS * g, V_ROWS)
            v = u[i, part, rows(h), :]
            a = pltpu.roll(v, nv - 1, 2) - v
            b = v - pltpu.roll(v, 1, 2)
            q1 = jnp.where(last, b, a)
            q0 = jnp.where(first, a, b)
            vq[i, h, part] = 3.0 * (q0 + q1)
            vd[i, h, part] = q1 - q0

        def level_1(i, h, g):
            part = pl.ds(V_ROWS * g, V_ROWS)
            d = vd[i, h, part]
            dm = pltpu.roll(d, 1, 2)
            s = d - dm
            c = (s * s + eps) + 0.75 * (d * dm)
            r = 1.5 * s
            p = c + r * d
            m = c - r * dm
            vs[i, h, part] = s
            vc[i, h, part] = c * c
            vp[i, h, part] = p * p
            vm[i, h, part] = m * m

        def level_2(i, h, g):
            part = pl.ds(V_ROWS * g, V_ROWS)
            s = vs[i, h, part]
            ta = s - pltpu.roll(s, 1, 2)
            tb = pltpu.roll(s, nv - 1, 2) - s
            p = pltpu.roll(vp[i, h, part], 1, 2)
            m = pltpu.roll(vm[i, h, part], nv - 1, 2)
            c = vc[i, h, part]
            left = one_side(jnp.where(first, e2, p), c, m, jnp.where(first, 0.0, ta), tb)
            right = one_side(jnp.where(first, e2, m), c, p, jnp.where(first, 0.0, tb), ta)
            vl[i, h, part] = left + s
            vr[i, h, part] = right - s

        def level_3(i, h, g):
            part = pl.ds(V_ROWS * g, V_ROWS)
            right = pltpu.roll(vr[i, h, part], nv - 1, 2)
            d3 = vq[i, h, part]
            acc[i, part, inner(h), :] = factor * jnp.maximum(d3 + right, vl[i, h, part] - d3)

        levels = (level_0, level_1, level_2, level_3)
        apart = V_APART
        for step in range(len(blocks) + apart * (len(levels) - 1)):
            for n in reversed(range(len(levels))):
                k = step - apart * n
                if 0 <= k < len(blocks):
                    levels[n](*blocks[k])

    def h_pass(s, h, g):
        u = us.at[s]
        factor = TURN_MAX / (6.0 * d_theta)

        def body(i, carry):
            cells = [hlo[s, h, i, k] for k in range(3)]
            cells += [u[i, k, rows(h), :] for k in range(nh)]
            cells += [hhi[s, h, i, k] for k in range(3)]
            d, sd, t, p, c, m = along(cells, eps_of(d_theta))
            square = lambda r: [None] + [e * e for e in r[1:]]
            p, c, m = square(p), square(c), square(m)
            sides = {}
            for k in range(2, nh + 3):
                sides[k] = both_sides(p[k - 1], c[k], m[k + 1], t[k - 1], t[k])
            for j in range(nh):
                k = j + 2
                d3 = 3.0 * (cells[j + 4] - cells[j + 2])
                value = jnp.maximum(d3 + (sides[k + 1][1] - sd[k + 1]), (sides[k][0] + sd[k]) - d3)
                acc[i, j, inner(h), :] += factor * value
            return carry

        lax.fori_loop(g * (nx // 2), (g + 1) * (nx // 2), body, 0, unroll=2)

    def x_pass(s, h, store):
        u = us.at[s]

        def body(j, carry):
            cells = [xlo[s, h, k, j] for k in range(3)]
            cells += [u[k, j, rows(h), :] for k in range(nx)]
            cells += [xhi[s, h, k, j] for k in range(3)]
            d, sd, t, p, c, m = along(cells, eps_of(CELL_SIZE))
            for i in range(nx):
                k = i + 2
                f2 = fx2[i, j, inner(h), :]
                ahead = f2 > 0.0
                b1 = jnp.where(ahead, m[k + 2], p[k - 1])
                b2 = jnp.where(ahead, c[k + 1], c[k])
                b3 = jnp.where(ahead, p[k], m[k + 1])
                t1 = jnp.where(ahead, t[k + 1], t[k - 1])
                dd = d[k] - jnp.where(ahead, d[k + 1], d[k - 1])
                fix = one_side(b1 * b1, b2 * b2, b3 * b3, t1, t[k])
                term = f2 * (cells[i + 4] - cells[i + 2]) + fx6[i, j, inner(h), :] * (dd + fix)
                store(i, j, h, acc[i, j, inner(h), :] + term)
            return carry

        lax.fori_loop(0, nh, body, 0, unroll=2)

    def y_term(u, i, j, h):
        eps = eps_of(CELL_SIZE)
        f2 = fy2[i, j, inner(h), :]
        ahead = f2 > 0.0
        cells = [u[i, j, pl.ds(8 + 8 * h + r, 8), :] for r in range(-3, 4)]
        q = [cells[k + 1] - cells[k] for k in range(6)]
        d = [q[k + 1] - q[k] for k in range(5)]
        e1 = jnp.where(ahead, d[4], d[0])
        e2 = jnp.where(ahead, d[3], d[1])
        e3 = d[2]
        e4 = jnp.where(ahead, d[1], d[3])
        s1, s2, s3 = e2 - e1, e3 - e2, e4 - e3
        e2k, e3k = 0.75 * e2, 0.75 * e3
        b1 = (s1 * s1 + eps) + e2k * (e2 + s1)
        b2 = (s2 * s2 + eps) + e2k * e3
        b3 = (s3 * s3 + eps) + e3k * (e3 - s3)
        fix = one_side(b1 * b1, b2 * b2, b3 * b3, s2 - s1, s3 - s2)
        return f2 * (cells[4] - cells[2]) + fy6[i, j, inner(h), :] * (s2 + fix)

    def add_up(i, j, h, total):
        acc[i, j, inner(h), :] = total

    def keep_rate(i, j, h, total):
        rate_0[i, j, inner(h), :] = jnp.minimum(total, 0.0)

    def y_first(h):
        def body(i, carry):
            for j in range(nh):
                acc[i, j, inner(h), :] += y_term(us.at[0], i, j, h)
            return carry

        lax.fori_loop(0, nx, body, 0, unroll=2)

    def pack_first(h):
        def body(i, carry):
            for j in range(nh):
                if h == 0:
                    ysend[1, 0, i, pl.ds(3 * j, 3), :] = rate_0[i, j, 0:3, :]
                if h == halves - 1:
                    ysend[1, 1, i, pl.ds(3 * j, 3), :] = rate_0[i, j, ny - 3:ny, :]
            return carry

        lax.fori_loop(0, nx, body, 0)

    def y_second(h):
        dt = 0.25 * step_buf[...]

        def body(i, carry):
            for j in range(nh):
                change = jnp.minimum(acc[i, j, inner(h), :] + y_term(us.at[1], i, j, h), 0.0)
                fresh = (0.75 * us[0, i, j, rows(h), :] + 0.25 * us[1, i, j, rows(h), :]) + dt * change
                us[2, i, j, rows(h), :] = fresh
                if h == 0:
                    ysend[2, 0, i, pl.ds(3 * j, 3), :] = fresh[0:3]
                if h == halves - 1:
                    ysend[2, 1, i, pl.ds(3 * j, 3), :] = fresh[5:8]
            return carry

        x_sent(1, h)
        h_sent(1, h)
        down, up = x_copies(2, h, field(2), base(2))
        for g in range(2):
            lax.fori_loop(g * (nx // 2), (g + 1) * (nx // 2), body, 0, unroll=2)
            for copy in h_copies(2, h, g, field(2), base(2)):
                copy.start()
            if g == 0:
                pl.when(below_x)(down.start)
            else:
                pl.when(above_x)(up.start)
        if h == 0:
            start_y(2, 0)
        if h == halves - 1:
            start_y(2, 1)

    def y_third(h):
        dt = step_buf[...]

        def body(i, carry):
            for j in range(nh):
                change = jnp.minimum(acc[i, j, inner(h), :] + y_term(us.at[2], i, j, h), 0.0)
                out_ref[i, j, inner(h), :] = (us[2, i, j, rows(h), :] - us[0, i, j, rows(h), :]) + dt * change
            return carry

        lax.fori_loop(0, nx, body, 0, unroll=2)

    def receive_x(s, h):
        u = us.at[s]
        down, up = x_copies(s, h)
        pl.when(above_x)(down.wait_recv)
        pl.when(below_x)(up.wait_recv)

        def stepped(halo):
            def body(k, carry):
                dt = step_buf[...]
                for j in range(nh):
                    halo[1, h, k, j] = halo[0, h, k, j] + dt * halo[1, h, k, j]
                return carry
            lax.fori_loop(0, 3, body, 0)

        pl.when(jnp.logical_and(s == 1, above_x))(lambda: stepped(xhi))
        pl.when(jnp.logical_and(s == 1, below_x))(lambda: stepped(xlo))

        @pl.when(jnp.logical_not(below_x))
        def _():
            def body(j, carry):
                edge = u[0, j, rows(h), :]
                slope = edge - u[1, j, rows(h), :]
                for r in (1, 2, 3):
                    xlo[s, h, 3 - r, j] = edge + float(r) * slope
                return carry
            lax.fori_loop(0, nh, body, 0)

        @pl.when(jnp.logical_not(above_x))
        def _():
            def body(j, carry):
                edge = u[nx - 1, j, rows(h), :]
                slope = edge - u[nx - 2, j, rows(h), :]
                for r in (1, 2, 3):
                    xhi[s, h, r - 1, j] = edge + float(r) * slope
                return carry
            lax.fori_loop(0, nh, body, 0)

    def receive_h(s, h, g):
        for copy in h_copies(s, h, g):
            copy.wait_recv()

        @pl.when(s == 1)
        def _():
            def body(i, carry):
                dt = step_buf[...]
                for k in range(3):
                    hlo[1, h, i, k] = hlo[0, h, i, k] + dt * hlo[1, h, i, k]
                    hhi[1, h, i, k] = hhi[0, h, i, k] + dt * hhi[1, h, i, k]
                return carry
            lax.fori_loop(g * (nx // 2), (g + 1) * (nx // 2), body, 0)

    def receive_y(s, which):
        u = us.at[s]
        copy = y_copies(s)[which]
        there = (above_y, below_y)[which]

        @pl.when(there)
        def _():
            copy.wait_recv()

            halo = (yhi, ylo)[which]
            place = pl.ds((8 + ny, 5)[which], 3)

            @pl.when(s == 1)
            def _():
                def body(i, carry):
                    halo[1, i] = halo[0, i] + step_buf[0:1, :] * halo[1, i]
                    return carry
                lax.fori_loop(0, nx, body, 0)

            def body(i, carry):
                for j in range(nh):
                    u[i, j, place, :] = halo[s, i, pl.ds(3 * j, 3), :]
                return carry
            lax.fori_loop(0, nx, body, 0)

        @pl.when(jnp.logical_not(there))
        def _():
            def body(i, carry):
                for j in range(nh):
                    if which == 0:
                        edge = u[i, j, pl.ds(8 + ny - 1, 1), :]
                        slope = edge - u[i, j, pl.ds(8 + ny - 2, 1), :]
                        for r in (1, 2, 3):
                            u[i, j, pl.ds(8 + ny - 1 + r, 1), :] = edge + float(r) * slope
                    else:
                        edge = u[i, j, pl.ds(8, 1), :]
                        slope = edge - u[i, j, pl.ds(9, 1), :]
                        for r in (1, 2, 3):
                            u[i, j, pl.ds(8 - r, 1), :] = edge + float(r) * slope
                return carry
            lax.fori_loop(0, nx, body, 0)

    def apply_step():
        top_all(1).wait_recv()
        best = top_send[1]
        for k in range(1, gy_n):
            best = jnp.maximum(best, top_y[k - 1])
        rate = best / CELL_SIZE + (TURN_MAX / d_theta + ACCEL_MAX / d_speed)
        dt = CFL_NUMBER / rate
        step_buf[...] = dt

        def body(i, carry):
            fresh = [us[0, i, j, rows(h), :] + dt * rate_0[i, j, inner(h), :] for j in range(nh) for h in range(halves)]
            for j in range(nh):
                for h in range(halves):
                    us[1, i, j, rows(h), :] = fresh[j * halves + h]
            return carry

        lax.fori_loop(0, nx, body, 0)

    def first_stage():
        for h in range(1, halves):
            start_half(0, h)
        top_all(0).wait_recv()
        best = top_send[0]
        for k in range(1, gx_n):
            best = jnp.maximum(best, top_x[k - 1])
        top_send[1] = best
        for copy in top_copies[1]:
            copy.start()
        receive_y(0, 0)
        receive_y(0, 1)
        for h in range(halves):
            y_first(h)
            for g in range(2):
                receive_h(0, h, g)
                h_pass(0, h, g)
            receive_x(0, h)
            x_pass(0, h, keep_rate)
            pack_first(h)
            start_half(1, h)
            if h == 0:
                start_y(1, 0)
            if h == halves - 1:
                start_y(1, 1)

    def later_stage(s):
        for h in range(halves):
            for g in range(2):
                receive_h(s, h, g)
                h_pass(s, h, g)
            receive_x(s, h)
            x_pass(s, h, add_up)
            if h == 0:
                receive_y(s, 1)
            if h == halves - 1:
                receive_y(s, 0)
            pl.when(s == 1)(lambda: y_second(h))
            pl.when(s == 2)(lambda: y_third(h))

    def stage(s, carry):
        pl.when(s == 1)(apply_step)
        v_pass(s)
        pl.when(s == 0)(first_stage)
        pl.when(s > 0)(lambda: later_stage(s))
        return carry

    lax.fori_loop(0, 3, stage, 0)

    top_all(0).wait_send()
    top_all(1).wait_send()
    for h in range(halves):
        x_sent(2, h)
        h_sent(2, h)
    y_sent(2, 0)
    y_sent(2, 1)


def solution(mesh):
    gx_n, gy_n, ha_n = mesh.shape["gx"], mesh.shape["gy"], mesh.shape["ha"]

    def body(level_set, wind_field):
        nx, ny, nh, nv = level_set.shape
        halves = ny // 8
        f32 = jnp.float32
        plain = pltpu.VMEM((nx, nh, ny, nv), f32)
        y_rows = -(-3 * nh // 8) * 8
        block_8 = pltpu.VMEM((nx, halves, nh, 8, nv), f32)
        dma = pltpu.SemaphoreType.DMA
        block = pltpu.with_memory_space_constraint(jnp.transpose(level_set, (0, 2, 1, 3)), pltpu.HBM)
        wind_field = pltpu.with_memory_space_constraint(wind_field, pltpu.HBM)
        out = pl.pallas_call(
            functools.partial(kernel, (gx_n, gy_n, ha_n, nx, nh, ny, nv)),
            out_shape=jax.ShapeDtypeStruct(block.shape, f32),
            in_specs=[
                pl.BlockSpec(memory_space=pltpu.HBM),
                pl.BlockSpec(memory_space=pltpu.HBM),
            ],
            out_specs=pl.BlockSpec(memory_space=pltpu.VMEM),
            scratch_shapes=[
                pltpu.VMEM((2, nx, ny), f32),
                pltpu.VMEM((3, nx, nh, ny + 16, nv), f32),
                plain,
                plain, plain, plain, plain, plain,
                pltpu.VMEM((3, halves, 3, nh, 8, nv), f32),
                pltpu.VMEM((3, halves, 3, nh, 8, nv), f32),
                pltpu.VMEM((3, halves, nx, 3, 8, nv), f32),
                pltpu.VMEM((3, halves, nx, 3, 8, nv), f32),
                pltpu.VMEM((3, nx, y_rows, nv), f32),
                pltpu.VMEM((3, nx, y_rows, nv), f32),
                pltpu.VMEM((3, 2, nx, y_rows, nv), f32),
                pltpu.VMEM((nh * ha_n, nv), f32),
                pltpu.VMEM((nh * ha_n, nv), f32),
                pltpu.VMEM((nx, ny, nv), f32),
                pltpu.VMEM((nx, ny, nv), f32),
                pltpu.VMEM((8, nv), f32),
                block_8, block_8, block_8, block_8, block_8, block_8, block_8, block_8,
                pltpu.VMEM((gx_n - 1, 8, nv), f32),
                pltpu.VMEM((gy_n - 1, 8, nv), f32),
                pltpu.VMEM((2, 8, nv), f32),
                dma((2,)),
                dma((halves, 2)), dma((2, halves, 2)),
                dma((halves, 2, 2)), dma((2, halves, 2, 2)),
                dma((2,)), dma((2, 2)),
                dma((2,)), dma((2,)),
            ],
            compiler_params=pltpu.CompilerParams(
                collective_id=0, has_side_effects=True, vmem_limit_bytes=VMEM_LIMIT),
        )(block, wind_field)
        return jnp.transpose(out * (2.0 / 3.0 / SCALE), (0, 2, 1, 3))

    return jax.shard_map(
        body,
        mesh=mesh,
        in_specs=(P("gx", "gy", "ha", None), P(None, "gx", "gy")),
        out_specs=P("gx", "gy", "ha", None),
        check_vma=False,
    )
```
